512 devices in a mesh: clip: 8 (over y), tm: 16 (over z_lo, x), mp: 4 (over z_hi, core).
Axes of the slice: x: 4, y: 8, z: 8 (z_hi: 2, z_lo: 4; z = z_hi * 4 + z_lo), core: 2. Of those that a mesh axis runs over, the one named last changes fastest.
Arguments:
- token_ids: int32 [128, 256], P(('clip', 'tm')), parts along dimension 0, may hold values from 0 to 1023
- remask: int32 [128, 256], P(('clip', 'tm')), parts along dimension 0, may hold values from -1 to 255, as said below
- position_embed: bfloat16 [16, 256, 1024], P('tm'), may hold values from -0.625 to 0.625
- mask_embed: bfloat16 [1024], replicated, may hold values from -0.625 to 0.625
- table: bfloat16 [1024, 1024], P('mp')
- gain_in: float32 [1024], replicated, may hold values from 0.5 to 1.5
- gain_out: float32 [1024], replicated, may hold values from 0.5 to 1.5
- w_qkv: bfloat16 [3, 1024, 1024], P(None, None, 'mp')
- w_out: bfloat16 [1024, 1024], P('mp'), may hold values from -0.1875 to 0.1875
Outputs:
- log_probs: bfloat16 [128, 256, 1024], P(('clip', 'tm'), None, 'mp'), parts along dimension 0
- confidence: float32 [128, 256], P(('clip', 'tm')), parts along dimension 0
- clip_stats: float32 [16], P('clip'), parts along dimension 0
The draws below stay inside these ranges and needn't reach their ends.
There are 8 independent parts, one for each index of `clip`. The reference program is written for one: setup_inputs(seed, part) draws one part's arguments, and reference() takes and returns one part's arrays. A program takes and returns all parts, laid end to end along the dimension named above; an argument that names none is the same for every part. Nothing has to cross between parts.
Inputs may be any that keep to these rules, and one draw needn't show every extreme that they name: `remask`: row f lists distinct masked positions of frame f in its first slots and -1 in the unused ones; every frame lists at least one position.
All inputs are finite; a program needn't handle non-finite values.
Results may differ from the reference program's by a relative error of at most 0.019.
The reference program's roundings to bfloat16 on the way (of `normed`, `context` and `final_rows`) count: a program that leaves them out, or rounds other values in their place, can miss the bound.
Values may be sent and summed in bfloat16 or wider, within the bound.
A program may use at most 64 MiB of HBM per device.

```python
import math
import jax
import jax.numpy as jnp
import numpy as np
from jax import lax

D = 1024
HEADS = 16
VOCAB = 1024
HEAD_DIM = 64
SPAN = 256
FRAMES = 16
TOKENS = 4096
SLOTS = 256


def draw_remask(key, part):
    pick_key = jax.random.fold_in(key, 3)
    spread_key = jax.random.fold_in(key, 5)
    steps_all = max(FRAMES - 1, 1)
    base_counts = [max(1, int(SPAN / 64.0 * 64.0 ** (frame / steps_all) + 0.5)) for frame in range(FRAMES)]
    live_count = jnp.array(base_counts, dtype=jnp.int32)
    live_count = live_count + jax.random.randint(spread_key, (FRAMES,), 0, SPAN // 64 + 1)
    live_count = jnp.minimum(live_count, SLOTS)
    scores = jax.random.randint(pick_key, (FRAMES, SPAN), 0, 65536) * SPAN + jnp.arange(SPAN, dtype=jnp.int32)[None, :]
    places = jnp.argsort(scores, axis=-1, stable=True).astype(jnp.int32)
    slot_ids = jnp.arange(SLOTS, dtype=jnp.int32)
    return jnp.where(slot_ids[None, :] < live_count[:, None], places, -1).astype(jnp.int32)


def draw_table(key, part):
    base = jax.random.normal(key, (VOCAB, D), jnp.float32) * 0.1
    return base.astype(jnp.bfloat16)


def draw_w_qkv(key, part):
    base = jax.random.normal(key, (3, D, D), jnp.float32) * D ** (-0.5)
    return base.astype(jnp.bfloat16)


def touch_ends(drawn, rng, smallest, high):
    shape = drawn.shape
    spot = [jax.random.randint(jax.random.fold_in(rng, axis), (), 0, shape[axis]) for axis in range(len(shape))]
    drawn = drawn.at[tuple(spot)].set(smallest)
    longest = shape.index(max(shape))
    spot[longest] = (spot[longest] + 1) % shape[longest]
    return drawn.at[tuple(spot)].set(high)


def shard_levels(rng, extent, split, low, largest):
    factor_of = 1.0
    for position, blocks in split:
        steps = jax.random.uniform(jax.random.fold_in(jax.random.fold_in(rng, 6), position), (blocks,), jnp.float32, low / len(split), largest / len(split))
        factor_of = factor_of * jnp.repeat(jnp.exp(steps), extent[position] // blocks).reshape((-1,) + (1,) * (len(extent) - 1 - position))
    return factor_of


def cumulative_ranks(amount, slope):
    weights = [(1 << 20) // math.isqrt(standing ** slope) + 1 for standing in range(1, amount + 1)]
    scale = 1 + sum(weights) // (1 << 30)
    return np.cumsum(np.array([max(1, weight // scale) for weight in weights]))


def ranked(key, shape, amount, lean):
    listing = cumulative_ranks(amount, lean)
    pick = jax.random.randint(jax.random.fold_in(key, 1), shape, 0, int(listing[amount - 1]))
    rank = jnp.searchsorted(jnp.asarray(listing, jnp.int32), pick, side="right")
    return jax.random.permutation(jax.random.fold_in(key, 2), amount)[rank].astype(jnp.int32)


def noise(own_key, shape, scale, reach, cuts=(), held_as=jnp.bfloat16):
    factor_of = shard_levels(own_key, shape, cuts, -0.22, 0.18) if cuts else 1.0
    values = jax.random.normal(own_key, shape, jnp.float32) * scale * factor_of
    return jnp.minimum(jnp.maximum(values, -reach), reach).astype(held_as)


def setup_inputs(seed: int = 0, part: int = 0) -> dict:
    arg_keys = jax.random.split(jax.random.key(seed), 10)
    own_keys = jax.random.split(jax.random.fold_in(arg_keys[9], part), 10)
    return {
        "token_ids": touch_ends(ranked(own_keys[0], (FRAMES, SPAN), VOCAB, 2), jax.random.fold_in(own_keys[0], 3), 0, VOCAB - 1).astype(jnp.int32),
        "remask": draw_remask(jax.random.fold_in(jax.random.fold_in(arg_keys[9], part), 71), part),
        "position_embed": noise(arg_keys[2], (FRAMES, SPAN, D), 0.1, 0.625, ((0, 16),)),
        "mask_embed": noise(arg_keys[3], (D,), 0.1, 0.625),
        "table": draw_table(jax.random.fold_in(arg_keys[9], 71), part),
        "gain_in": jnp.clip(1.0 + 0.1 * jax.random.normal(arg_keys[5], (D,), jnp.float32), 0.5, 1.5),
        "gain_out": jnp.clip(1.0 + 0.1 * jax.random.normal(arg_keys[6], (D,), jnp.float32), 0.5, 1.5),
        "w_qkv": draw_w_qkv(jax.random.fold_in(arg_keys[9], 71), part),
        "w_out": noise(arg_keys[8], (D, D), D ** -0.5, 0.1875, ((0, 4),)),
    }


def layer_norm(values, gain):
    center = values - lax.optimization_barrier(jnp.mean(values, axis=-1, keepdims=True))
    spread = lax.optimization_barrier(jnp.mean(center * center, axis=-1, keepdims=True))
    return center * lax.rsqrt(spread + 1e-05) * gain

def attend_head(trio):
    query, keys, values = trio
    blocks = query.reshape(FRAMES, SPAN, HEAD_DIM)

    def one_block(block):
        scores = jnp.dot(block, keys.T, preferred_element_type=jnp.float32) * HEAD_DIM ** (-0.5)
        highest = lax.optimization_barrier(jnp.max(scores, axis=-1, keepdims=True))
        weights = jnp.exp(scores - highest)
        summed = jnp.dot(weights.astype(jnp.bfloat16), values, preferred_element_type=jnp.float32)
        return summed / lax.optimization_barrier(jnp.sum(weights, axis=-1, keepdims=True))
    return lax.map(one_block, blocks).reshape(TOKENS, HEAD_DIM)

def reference(token_ids, remask, position_embed, mask_embed, table, gain_in, gain_out, w_qkv, w_out):
    positions = jnp.arange(SPAN, dtype=jnp.int32)
    masked = jnp.any(remask[:, None, :] == positions[None, :, None], axis=-1)
    looked = jnp.take(table, token_ids, axis=0).astype(jnp.float32)
    hidden_in = jnp.where(masked[:, :, None], mask_embed.astype(jnp.float32)[None, None, :], looked)
    hidden_in = (hidden_in + position_embed.astype(jnp.float32)).reshape(TOKENS, D)
    normed = layer_norm(hidden_in, gain_in).astype(jnp.bfloat16)
    query = jnp.dot(normed, w_qkv[0], preferred_element_type=jnp.float32).astype(jnp.bfloat16)
    keys = jnp.dot(normed, w_qkv[1], preferred_element_type=jnp.float32).astype(jnp.bfloat16)
    values = jnp.dot(normed, w_qkv[2], preferred_element_type=jnp.float32).astype(jnp.bfloat16)
    heads_query = query.reshape(TOKENS, HEADS, HEAD_DIM).transpose(1, 0, 2)
    heads_keys = keys.reshape(TOKENS, HEADS, HEAD_DIM).transpose(1, 0, 2)
    heads_values = values.reshape(TOKENS, HEADS, HEAD_DIM).transpose(1, 0, 2)
    context = lax.map(attend_head, (heads_query, heads_keys, heads_values))
    context = context.transpose(1, 0, 2).reshape(TOKENS, D).astype(jnp.bfloat16)
    mixed_rows = jnp.dot(context, w_out, preferred_element_type=jnp.float32)
    final_rows = layer_norm(hidden_in + mixed_rows, gain_out).astype(jnp.bfloat16)
    logits = jnp.dot(final_rows, table.T, preferred_element_type=jnp.float32)
    highest = lax.optimization_barrier(jnp.max(logits, axis=-1, keepdims=True))
    log_total = highest + jnp.log(lax.optimization_barrier(jnp.sum(jnp.exp(logits - highest), axis=-1, keepdims=True)))
    log_probs = (logits - log_total).astype(jnp.bfloat16).reshape(FRAMES, SPAN, VOCAB)
    confidence = jnp.exp(highest - log_total).reshape(TOKENS)
    weight = masked.reshape(TOKENS).astype(jnp.float32)
    count = jnp.sum(weight)
    clip_stats = jnp.stack([jnp.sum(confidence * weight) / count, jnp.log(count / TOKENS)])
    return (log_probs, confidence.reshape(FRAMES, SPAN), clip_stats)
```

```python
import math

import jax
import jax.numpy as jnp
from jax import lax
from jax.experimental import pallas as pl
from jax.experimental.pallas import tpu as pltpu
from jax.sharding import Mesh
from jax.sharding import PartitionSpec as P

HEAD_DIM = 64
MESH = pl.DeviceIdType.MESH
AXES = ("clip", "zl", "x", "zh", "core")
BF = jnp.bfloat16
F32 = jnp.float32
SCALE = HEAD_DIM**-0.5 * math.log2(math.e)


def coords():
    return [lax.axis_index(name) for name in AXES]


def at(y, zl, x, zh, core):
    mine = coords()
    sizes = (8, 4, 4, 2, 2)
    return tuple(
        lax.rem(mine[k] + step + sizes[k], sizes[k]) if step else mine[k]
        for k, step in enumerate((y, zl, x, zh, core))
    )


def mirror():
    y, zl, x, zh, core = coords()
    return (y, 3 - zl, x, 1 - zh, core)


def remote(src, dst, send, recv, device):
    return pltpu.make_async_remote_copy(
        src_ref=src, dst_ref=dst, send_sem=send, recv_sem=recv, device_id=device, device_id_type=MESH
    )


def arrived(ref, sem):
    remote(ref, ref, sem, sem, at(0, 0, 0, 0, 1)).wait_recv()


def left(ref, sem):
    remote(ref, ref, sem, sem, at(0, 0, 0, 0, 1)).wait_send()


def norm_rows(h, gain):
    center = h - jnp.mean(h, axis=-1, keepdims=True)
    spread = jnp.mean(center * center, axis=-1, keepdims=True)
    return center * lax.rsqrt(spread + 1e-05) * gain


class Spread:
    def __init__(self, hbm, full, ssem, zsem, ysem, xsem, dsem):
        self.hbm, self.full = hbm, full
        self.ssem, self.zsem, self.ysem, self.xsem, self.dsem = ssem, zsem, ysem, xsem, dsem
        y, zl, x, zh, core = coords()
        self.y, self.x = y, x
        self.own = zh * 2 + core
        self.got = (1 - zh) * 2 + core

    def rows(self, quarter, x):
        return pl.ds(pl.multiple_of(quarter * 256 + x * 64, 64), 64)

    def cols(self, y):
        return pl.ds(pl.multiple_of(y * 128, 128), 128)

    def local(self):
        quarter = pl.ds(pl.multiple_of(self.own * 256, 256), 256)
        return pltpu.make_async_copy(self.hbm, self.full.at[quarter], self.ssem.at[4])

    def start_z(self):
        src = self.hbm.at[pl.ds(pl.multiple_of(self.x * 64, 64), 64), self.cols(self.y)]
        dst = self.full.at[self.rows(self.own, self.x), self.cols(self.y)]
        remote(src, dst, self.ssem.at[0], self.zsem, mirror()).start()

    def start_own_quarter(self):
        quarter = pl.ds(pl.multiple_of(self.own * 256, 256), 256)
        remote(
            self.hbm, self.full.at[quarter], self.ssem.at[3], self.dsem.at[0], at(0, 0, 0, 0, 1)
        ).start()

    def forward_x(self, y):
        piece = self.full.at[self.rows(self.got, self.x), self.cols(y)]
        for dx in (1, 3, 2):
            remote(piece, piece, self.ssem.at[2], self.xsem.at[dx], at(0, 0, dx, 0, 0)).start()

    def start_y(self):
        piece = self.full.at[self.rows(self.got, self.x), self.cols(self.y)]
        arrived(piece, self.zsem)
        for dy in (4, 3, 5, 2, 6, 1, 7):
            remote(piece, piece, self.ssem.at[1], self.ysem.at[dy], at(dy, 0, 0, 0, 0)).start()
        self.forward_x(self.y)

    def start_x(self):
        for dy in (1, 7, 2, 6, 3, 5, 4):
            source = lax.rem(self.y - dy + 8, 8)
            piece = self.full.at[self.rows(self.got, self.x), self.cols(source)]
            arrived(piece, self.ysem.at[dy])
            self.forward_x(source)
        self.hand_over(self.x)

    def hand_over(self, x):
        block = self.full.at[self.rows(self.got, x)]
        remote(block, block, self.ssem.at[3], self.dsem.at[1], at(0, 0, 0, 0, 1)).start()

    def finish_x(self):
        for dx in (1, 3, 2):
            x = lax.rem(self.x - dx + 4, 4)
            arrived(self.full.at[self.rows(self.got, x)], self.xsem.at[dx])
            self.hand_over(x)

    def wait_all(self):
        quarter = self.full.at[pl.ds(0, 256)]
        arrived(quarter, self.dsem.at[0])
        arrived(quarter, self.dsem.at[1])

    def wait_sent(self):
        left(self.full.at[pl.ds(0, 64), pl.ds(0, 128)], self.ssem.at[0])
        left(self.full.at[pl.ds(0, 64), pl.ds(0, 896)], self.ssem.at[1])
        left(self.full.at[pl.ds(0, 192)], self.ssem.at[2])
        left(self.full.at[pl.ds(0, 512)], self.ssem.at[3])


def kernel(
    ids_ref, remask_ref, mask_embed_ref, gain_in_ref, gain_out_ref, table_hbm, wqkv_hbm, wout_hbm, pos_hbm,
    logp_ref, conf_ref, stats_ref,
    table, wout, wqkv, pos, hidden, normed, kv_out, q_out, kv, q_in, qpad, high, total, summed, o_out, ctx,
    final, logits, weight, stat_out, stat_in,
    local_sem, t_s, t_z, t_y, t_x, t_d, w_s, w_z, w_y, w_x, w_d, a_send, a_recv, q_recv, b_send, b_recv,
    c_send, c_recv, f_send, f_recv, s_send, s_recv,
):
    y, zl, x, zh, core = coords()
    mp = zh * 2 + core
    frame = zl * 4 + x
    tab = Spread(table_hbm, table, t_s, t_z, t_y, t_x, t_d)
    out = Spread(wout_hbm, wout, w_s, w_z, w_y, w_x, w_d)
    load_pos = pltpu.make_async_copy(pos_hbm.at[0], pos, local_sem.at[0])
    load_qkv = pltpu.make_async_copy(wqkv_hbm, wqkv, local_sem.at[1])

    barrier = pltpu.get_barrier_semaphore()
    peers = []
    for k in range(1, 16):
        place = lax.rem(zh * 8 + zl * 2 + core + k, 16)
        peers.append((y, lax.rem(place // 2, 4), x, place // 8, lax.rem(place, 2)))
    peers += [at(k, 0, 0, 0, 0) for k in range(1, 8)]
    peers += [at(0, dz, dx, 0, 0) for dx in range(1, 4) for dz in range(4)]
    for peer in peers:
        pl.semaphore_signal(barrier, inc=1, device_id=peer, device_id_type=MESH)
    tab.local().start()
    load_pos.start()
    load_qkv.start()
    out.local().start()

    row = lax.broadcasted_iota(jnp.int32, (256, 256), 0)
    lane = lax.broadcasted_iota(jnp.int32, (256, 256), 1)
    masked = jnp.max(jnp.where(remask_ref[...] == row, 1.0, 0.0), axis=1, keepdims=True)
    ids_col = jnp.sum(
        jnp.where(row == lane, ids_ref[...].astype(F32), 0.0), axis=1, keepdims=True
    )
    weight[...] = jnp.broadcast_to(masked, (256, 128))
    entry = lax.broadcasted_iota(jnp.int32, (256, 1024), 1).astype(F32)
    onehot = jnp.where(entry == jnp.where(masked > 0.5, -1.0, ids_col), 1.0, 0.0).astype(BF)

    pl.semaphore_wait(barrier, len(peers))
    tab.start_z()
    out.start_z()
    tab.start_own_quarter()
    tab.start_y()
    out.start_y()
    tab.start_x()
    tab.finish_x()
    out.start_own_quarter()
    out.start_x()
    tab.local().wait()
    load_pos.wait()
    load_qkv.wait()
    tab.wait_all()

    hidden[...] = jnp.dot(onehot, table[...], preferred_element_type=F32)
    mask_row = mask_embed_ref[...].astype(F32)
    gain_in = gain_in_ref[...]

    def first_norm(k, carry):
        block = pl.ds(pl.multiple_of(k * 64, 64), 64)
        h = hidden[block] + jnp.where(weight[block][:, :1] > 0.5, mask_row, 0.0)
        h = h + pos[block].astype(F32)
        hidden[block] = h
        normed[block] = norm_rows(h, gain_in).astype(BF)
        return carry

    lax.fori_loop(0, 4, first_norm, 0)
    low = lax.broadcasted_iota(jnp.int32, (256, 128), 1) < 64
    n_all = normed[...]
    keys = jnp.dot(n_all, wqkv[1], preferred_element_type=F32)
    values = jnp.dot(n_all, wqkv[2], preferred_element_type=F32)
    for g in range(2):
        kg, vg = keys[:, g * 128 : g * 128 + 128], values[:, g * 128 : g * 128 + 128]
        kv_out[2 * g] = jnp.where(low, kg, pltpu.roll(vg, 64, 1)).astype(BF)
        kv_out[2 * g + 1] = jnp.where(low, pltpu.roll(kg, 64, 1), vg).astype(BF)
    query = jnp.dot(n_all, wqkv[0], preferred_element_type=F32)
    low_half = low[:128]
    for g in range(2):
        qa, qb = query[:128, g * 128 : g * 128 + 128], query[128:, g * 128 : g * 128 + 128]
        q_out[2 * g] = jnp.where(low_half, qa, pltpu.roll(qb, 64, 1)).astype(BF)
        q_out[2 * g + 1] = jnp.where(low_half, pltpu.roll(qa, 64, 1), qb).astype(BF)
    for dz in (1, 3, 2):
        head = lax.rem(zl + dz, 4)
        remote(
            kv_out.at[head], kv.at[0, 4 - dz], a_send.at[0], a_recv.at[4 - dz], at(0, dz, 0, 0, 0)
        ).start()
    for dx in (1, 3):
        remote(
            kv_out.at[zl], kv.at[1 if dx == 1 else 2, 0], b_send.at[0],
            b_recv.at[1 if dx == 1 else 2, 0], at(0, 0, dx, 0, 0),
        ).start()
    for dz in (1, 3, 2):
        head = lax.rem(zl + dz, 4)
        remote(
            q_out.at[head], q_in.at[4 - dz], a_send.at[1], q_recv.at[4 - dz], at(0, dz, 0, 0, 0)
        ).start()
    kv[0, 0] = kv_out[zl]

    def unpack(k, packed):
        packed = packed.astype(F32)
        qpad[k, :128] = jnp.where(low_half, packed, 0.0).astype(BF)
        qpad[k, 128:] = jnp.where(low_half, pltpu.roll(packed, 64, 1), 0.0).astype(BF)

    unpack(0, q_out[zl])
    out.finish_x()
    for s in (1, 3, 2):
        arrived(kv.at[0, s], a_recv.at[s])
        for dx in (1, 3):
            slot = 1 if dx == 1 else 2
            remote(
                kv.at[0, s], kv.at[slot, s], b_send.at[0], b_recv.at[slot, s], at(0, 0, dx, 0, 0)
            ).start()
    for s in (1, 3, 2):
        arrived(q_in.at[s], q_recv.at[s])
        unpack(s, q_in[s])

    def score(k, b):
        rows = kv[k].reshape(1024, 128)
        s = lax.dot_general(
            qpad[b], rows, (((1,), (1,)), ((), ())), preferred_element_type=F32
        )
        return rows, s, jnp.max(s, axis=1, keepdims=True)

    def first_block(b, carry):
        rows, s, top = score(0, b)
        w = jnp.exp2(s * SCALE - top * SCALE)
        high[b] = jnp.broadcast_to(top, (256, 128))
        total[b] = jnp.broadcast_to(jnp.sum(w, axis=1, keepdims=True), (256, 128))
        summed[b] = jnp.dot(w.astype(BF), rows, preferred_element_type=F32)
        return carry

    def next_block(k, b):
        rows, s, top = score(k, b)
        before = high[b]
        now = jnp.maximum(before, top)
        fade = jnp.exp2((before - now) * SCALE)
        w = jnp.exp2(s * SCALE - now[:, :1] * SCALE)
        sums = total[b] * fade + jnp.sum(w, axis=1, keepdims=True)
        acc = summed[b] * fade + jnp.dot(w.astype(BF), rows, preferred_element_type=F32)
        return now, sums, acc

    def later_block(k):
        def go(b, carry):
            high[b], total[b], summed[b] = next_block(k, b)
            return carry

        return go

    def relay(slot, s):
        arrived(kv.at[slot, s], b_recv.at[slot, s])
        remote(
            kv.at[slot, s], kv.at[3, s], b_send.at[0], b_recv.at[3, s], at(0, 0, 1 if slot == 1 else 3, 0, 0)
        ).start()

    relay(1, 0)
    relay(2, 1)
    lax.fori_loop(0, 4, first_block, 0)
    relay(2, 3)
    relay(1, 2)
    for s in (1, 3):
        arrived(kv.at[1, s], b_recv.at[1, s])
    lax.fori_loop(0, 4, later_block(1), 0)
    for s in (0, 2):
        arrived(kv.at[2, s], b_recv.at[2, s])
    lax.fori_loop(0, 4, later_block(2), 0)
    for s in range(4):
        arrived(kv.at[3, s], b_recv.at[3, s])
    low64 = low[:64]
    head_here = mp * 4 + zl
    for b in range(4):
        now, sums, acc = next_block(3, b)
        rows = acc / sums
        for half in range(2):
            top_rows = rows[half * 128 : half * 128 + 64]
            low_rows = rows[half * 128 + 64 : half * 128 + 128]
            o_out[b, half] = jnp.where(low64, pltpu.roll(top_rows, 64, 1), low_rows).astype(BF)
        for dh in range(2):
            for dc in range(2):
                if b == 0 and dh == 0 and dc == 0:
                    continue
                half = lax.rem(core + dc, 2)
                remote(
                    o_out.at[b, half], ctx.at[head_here], c_send.at[0], c_recv.at[0], at(0, b, 0, dh, dc)
                ).start()
    ctx[head_here] = o_out[0, core]
    out.local().wait()
    out.wait_all()
    arrived(ctx.at[pl.ds(0, 15)], c_recv.at[0])

    pieces = []
    for g in range(8):
        a, b = ctx[2 * g].astype(F32), ctx[2 * g + 1].astype(F32)
        pieces.append(
            jnp.concatenate(
                [
                    jnp.where(low64, a, pltpu.roll(b, 64, 1)),
                    jnp.where(low64, pltpu.roll(a, 64, 1), b),
                ],
                axis=0,
            ).astype(BF)
        )
    context = jnp.concatenate(pieces, axis=1)
    mine = pl.ds(pl.multiple_of(core * 128, 128), 128)
    h = hidden[mine] + jnp.dot(context, wout[...], preferred_element_type=F32)
    final[mine] = norm_rows(h, gain_out_ref[...]).astype(BF)
    send_final = remote(final.at[mine], final.at[mine], f_send.at[0], f_recv.at[0], at(0, 0, 0, 0, 1))
    send_final.start()

    def finish(block):
        rows = final[block]
        tops = []
        for q in range(4):
            part = lax.dot_general(
                rows, table[q * 256 : q * 256 + 256], (((1,), (1,)), ((), ())), preferred_element_type=F32
            )
            logits[q, block] = part
            tops.append(jnp.max(part, axis=1, keepdims=True))
        top = jnp.maximum(jnp.maximum(tops[0], tops[1]), jnp.maximum(tops[2], tops[3]))
        sums = jnp.zeros_like(top)
        for q in range(4):
            sums = sums + jnp.sum(jnp.exp(logits[q, block] - top), axis=1, keepdims=True)
        lse = top + jnp.log(sums)
        logp_ref[0, block] = (logits[mp, block] - lse).astype(BF)
        qpad_conf = jnp.exp(top - lse)
        high[0, block] = jnp.broadcast_to(qpad_conf, (128, 128))

    finish(mine)
    other = pl.ds(pl.multiple_of((1 - core) * 128, 128), 128)
    arrived(final.at[other], f_recv.at[0])
    finish(other)
    conf = high[0][:, :1]
    w = weight[...][:, :1]
    conf_sum = jnp.sum(conf * w, axis=0, keepdims=True)
    count = jnp.sum(w, axis=0, keepdims=True)
    lane8 = lax.broadcasted_iota(jnp.int32, (8, 128), 1)
    tile = jnp.where(lane8 == 0, conf_sum, jnp.where(lane8 == 1, count, 0.0))
    stat_out[...] = tile
    stat_in[frame] = tile
    conf_ref[...] = jnp.sum(jnp.where(row == lane, conf, 0.0), axis=0, keepdims=True)
    for dz in range(4):
        for dx in range(4):
            if dz or dx:
                remote(
                    stat_out, stat_in.at[frame], s_send.at[0], s_recv.at[0], at(0, dz, dx, 0, 0)
                ).start()
    tab.wait_sent()
    out.wait_sent()
    left(kv_out.at[pl.ds(0, 3)], a_send.at[0])
    left(q_out.at[pl.ds(0, 3)], a_send.at[1])
    left(kv.at[pl.ds(0, 3)], b_send.at[0])
    left(ctx.at[pl.ds(0, 15)], c_send.at[0])
    send_final.wait_send()
    arrived(stat_in.at[pl.ds(0, 15)], s_recv.at[0])
    left(stat_in.at[pl.ds(0, 15)], s_send.at[0])
    sums = stat_in[0]
    for k in range(1, 16):
        sums = sums + stat_in[k]
    sums = sums[:1]
    lane1 = lane8[:1]
    all_conf = jnp.sum(jnp.where(lane1 == 0, sums, 0.0), axis=1, keepdims=True)
    all_count = jnp.sum(jnp.where(lane1 == 1, sums, 0.0), axis=1, keepdims=True)
    stats_ref[...] = jnp.where(lane1 == 0, all_conf / all_count, jnp.log(all_count / 4096.0))


def body(token_ids, remask, position_embed, mask_embed, table, gain_in, gain_out, w_qkv, w_out):
    vmem = pl.BlockSpec(memory_space=pltpu.VMEM)
    hbm = pl.BlockSpec(memory_space=pl.ANY)
    dma = pltpu.SemaphoreType.DMA
    spread_sems = [dma((5,)), dma, dma((8,)), dma((4,)), dma((2,))]
    log_probs, confidence, stats = pl.pallas_call(
        kernel,
        out_shape=(
            jax.ShapeDtypeStruct((1, 256, 256), BF),
            jax.ShapeDtypeStruct((1, 256), F32),
            jax.ShapeDtypeStruct((1, 128), F32),
        ),
        in_specs=[vmem] * 5 + [hbm] * 4,
        out_specs=(vmem, vmem, vmem),
        scratch_shapes=[
            pltpu.VMEM((1024, 1024), BF),
            pltpu.VMEM((1024, 1024), BF),
            pltpu.VMEM((3, 1024, 256), BF),
            pltpu.VMEM((256, 1024), BF),
            pltpu.VMEM((256, 1024), F32),
            pltpu.VMEM((256, 1024), BF),
            pltpu.VMEM((4, 256, 128), BF),
            pltpu.VMEM((4, 128, 128), BF),
            pltpu.VMEM((4, 4, 256, 128), BF),
            pltpu.VMEM((4, 128, 128), BF),
            pltpu.VMEM((4, 256, 128), BF),
            pltpu.VMEM((4, 256, 128), F32),
            pltpu.VMEM((4, 256, 128), F32),
            pltpu.VMEM((4, 256, 128), F32),
            pltpu.VMEM((4, 2, 64, 128), BF),
            pltpu.VMEM((16, 64, 128), BF),
            pltpu.VMEM((256, 1024), BF),
            pltpu.VMEM((4, 256, 256), F32),
            pltpu.VMEM((256, 128), F32),
            pltpu.VMEM((8, 128), F32),
            pltpu.VMEM((16, 8, 128), F32),
            dma((2,)),
            *spread_sems,
            *spread_sems,
            dma((2,)),
            dma((4,)),
            dma((4,)),
            dma((1,)),
            dma((4, 4)),
            dma((1,)),
            dma((1,)),
            dma((1,)),
            dma((1,)),
            dma((1,)),
            dma((1,)),
        ],
        compiler_params=pltpu.CompilerParams(
            collective_id=0, has_side_effects=True, vmem_limit_bytes=60 * 1024 * 1024
        ),
        name="predict",
    )(
        token_ids,
        remask,
        mask_embed.reshape(1, -1),
        gain_in.reshape(1, -1),
        gain_out.reshape(1, -1),
        table,
        w_qkv,
        w_out,
        position_embed,
    )
    return log_probs, confidence, stats[0, :2]


def solution(mesh):
    finer = Mesh(mesh.devices.reshape(8, 4, 4, 2, 2), AXES)
    frames = ("clip", "zl", "x")
    tm = ("zl", "x")
    mp = ("zh", "core")
    in_specs = (
        P(frames, None),
        P(frames, None),
        P(tm, None, None),
        P(),
        P(mp, None),
        P(),
        P(),
        P(None, None, mp),
        P(mp, None),
    )
    out_specs = (P(frames, None, mp), P(frames, None), P("clip"))
    return jax.shard_map(body, mesh=finer, in_specs=in_specs, out_specs=out_specs, check_vma=False)
```

```python
import math

import jax
import jax.numpy as jnp
from jax import lax
from jax.experimental import pallas as pl
from jax.experimental.pallas import tpu as pltpu
from jax.sharding import Mesh
from jax.sharding import PartitionSpec as P

HEAD_DIM = 64
MESH = pl.DeviceIdType.MESH
AXES = ("clip", "zl", "x", "zh", "core")
BF = jnp.bfloat16
F32 = jnp.float32
SCALE = HEAD_DIM**-0.5 * math.log2(math.e)


def coords():
    return [lax.axis_index(name) for name in AXES]


def at(y, zl, x, zh, core):
    mine = coords()
    sizes = (8, 4, 4, 2, 2)
    return tuple(
        lax.rem(mine[k] + step + sizes[k], sizes[k]) if step else mine[k]
        for k, step in enumerate((y, zl, x, zh, core))
    )


def mirror():
    y, zl, x, zh, core = coords()
    return (y, 3 - zl, x, 1 - zh, core)


def remote(src, dst, send, recv, device):
    return pltpu.make_async_remote_copy(
        src_ref=src, dst_ref=dst, send_sem=send, recv_sem=recv, device_id=device, device_id_type=MESH
    )


def arrived(ref, sem):
    remote(ref, ref, sem, sem, at(0, 0, 0, 0, 1)).wait_recv()


def left(ref, sem):
    remote(ref, ref, sem, sem, at(0, 0, 0, 0, 1)).wait_send()


def norm_rows(h, gain):
    center = h - jnp.mean(h, axis=-1, keepdims=True)
    spread = jnp.mean(center * center, axis=-1, keepdims=True)
    return center * lax.rsqrt(spread + 1e-05) * gain


class Spread:
    def __init__(self, hbm, full, ssem, zsem, ysem, xsem, dsem):
        self.hbm, self.full = hbm, full
        self.ssem, self.zsem, self.ysem, self.xsem, self.dsem = ssem, zsem, ysem, xsem, dsem
        y, zl, x, zh, core = coords()
        self.y, self.x = y, x
        self.own = zh * 2 + core
        self.got = (1 - zh) * 2 + core

    def rows(self, quarter, x):
        return pl.ds(pl.multiple_of(quarter * 256 + x * 64, 64), 64)

    def cols(self, y):
        return pl.ds(pl.multiple_of(y * 128, 128), 128)

    def local(self):
        quarter = pl.ds(pl.multiple_of(self.own * 256, 256), 256)
        return pltpu.make_async_copy(self.hbm, self.full.at[quarter], self.ssem.at[4])

    def start_z(self):
        piece = self.full.at[self.rows(self.own, self.x), self.cols(self.y)]
        remote(piece, piece, self.ssem.at[0], self.zsem, mirror()).start()

    def start_own_quarter(self):
        quarter = pl.ds(pl.multiple_of(self.own * 256, 256), 256)
        remote(
            self.hbm, self.full.at[quarter], self.ssem.at[3], self.dsem.at[0], at(0, 0, 0, 0, 1)
        ).start()

    def forward_x(self, y):
        piece = self.full.at[self.rows(self.got, self.x), self.cols(y)]
        for dx in (1, 3, 2):
            remote(piece, piece, self.ssem.at[2], self.xsem.at[dx], at(0, 0, dx, 0, 0)).start()

    def start_y(self):
        piece = self.full.at[self.rows(self.got, self.x), self.cols(self.y)]
        arrived(piece, self.zsem)
        for dy in (4, 3, 5, 2, 6, 1, 7):
            remote(piece, piece, self.ssem.at[1], self.ysem.at[dy], at(dy, 0, 0, 0, 0)).start()
        self.forward_x(self.y)

    def start_x(self):
        for dy in (1, 7, 2, 6, 3, 5, 4):
            source = lax.rem(self.y - dy + 8, 8)
            piece = self.full.at[self.rows(self.got, self.x), self.cols(source)]
            arrived(piece, self.ysem.at[dy])
            self.forward_x(source)
        self.hand_over(self.x)

    def hand_over(self, x):
        block = self.full.at[self.rows(self.got, x)]
        remote(block, block, self.ssem.at[3], self.dsem.at[1], at(0, 0, 0, 0, 1)).start()

    def finish_x(self):
        for dx in (1, 3, 2):
            x = lax.rem(self.x - dx + 4, 4)
            arrived(self.full.at[self.rows(self.got, x)], self.xsem.at[dx])
            self.hand_over(x)

    def start_x_first(self):
        piece = self.full.at[self.rows(self.got, self.x), self.cols(self.y)]
        arrived(piece, self.zsem)
        for dx in (2, 1, 3):
            remote(piece, piece, self.ssem.at[2], self.xsem.at[dx], at(0, 0, dx, 0, 0)).start()

    def strip(self, y):
        return self.full.at[pl.ds(pl.multiple_of(self.got * 256, 256), 256), self.cols(y)]

    def start_y_second(self):
        for dx in (1, 3, 2):
            x = lax.rem(self.x - dx + 4, 4)
            arrived(self.full.at[self.rows(self.got, x), self.cols(self.y)], self.xsem.at[dx])
        strip = self.strip(self.y)
        for dy in (4, 3, 5, 2, 6, 1, 7):
            remote(strip, strip, self.ssem.at[1], self.ysem.at[dy], at(dy, 0, 0, 0, 0)).start()

    def finish_y_second(self):
        for dy in (1, 7, 2, 6, 3, 5, 4):
            arrived(self.strip(lax.rem(self.y - dy + 8, 8)), self.ysem.at[dy])
        quarter = self.full.at[pl.ds(pl.multiple_of(self.got * 256, 256), 256)]
        remote(quarter, quarter, self.ssem.at[3], self.dsem.at[1], at(0, 0, 0, 0, 1)).start()

    def wait_sent_x_first(self):
        left(self.full.at[pl.ds(0, 64), pl.ds(0, 128)], self.ssem.at[0])
        left(self.full.at[pl.ds(0, 256), pl.ds(0, 896)], self.ssem.at[1])
        left(self.full.at[pl.ds(0, 64), pl.ds(0, 384)], self.ssem.at[2])
        left(self.full.at[pl.ds(0, 512)], self.ssem.at[3])

    def wait_all(self):
        quarter = self.full.at[pl.ds(0, 256)]
        arrived(quarter, self.dsem.at[0])
        arrived(quarter, self.dsem.at[1])

    def wait_sent(self):
        left(self.full.at[pl.ds(0, 64), pl.ds(0, 128)], self.ssem.at[0])
        left(self.full.at[pl.ds(0, 64), pl.ds(0, 896)], self.ssem.at[1])
        left(self.full.at[pl.ds(0, 192)], self.ssem.at[2])
        left(self.full.at[pl.ds(0, 512)], self.ssem.at[3])


def kernel(
    ids_ref, remask_ref, mask_embed_ref, gain_in_ref, gain_out_ref, table_hbm, wqkv_hbm, wout_hbm, pos_hbm,
    logp_ref, conf_ref, stats_ref,
    table, wout, wqkv, pos, hidden, normed, kv_out, q_out, kv, q_in, qpad, high, total, summed, o_out, ctx,
    final, logits, weight, stat_out, stat_in,
    local_sem, t_s, t_z, t_y, t_x, t_d, w_s, w_z, w_y, w_x, w_d, a_send, a_recv, q_recv, b_send, b_recv,
    c_send, c_recv, f_send, f_recv, s_send, s_recv,
):
    y, zl, x, zh, core = coords()
    mp = zh * 2 + core
    frame = zl * 4 + x
    tab = Spread(table_hbm, table, t_s, t_z, t_y, t_x, t_d)
    out = Spread(wout_hbm, wout, w_s, w_z, w_y, w_x, w_d)
    load_pos = pltpu.make_async_copy(pos_hbm.at[0], pos, local_sem.at[0])
    load_qkv = pltpu.make_async_copy(wqkv_hbm, wqkv, local_sem.at[1])

    barrier = pltpu.get_barrier_semaphore()
    peers = []
    for k in range(1, 16):
        place = lax.rem(zh * 8 + zl * 2 + core + k, 16)
        peers.append((y, lax.rem(place // 2, 4), x, place // 8, lax.rem(place, 2)))
    peers += [at(k, 0, 0, 0, 0) for k in range(1, 8)]
    peers += [at(0, dz, dx, 0, dc) for dx in range(1, 4) for dz in range(4) for dc in range(2)]
    for peer in peers:
        pl.semaphore_signal(barrier, inc=1, device_id=peer, device_id_type=MESH)
    tab.local().start()
    load_pos.start()
    load_qkv.start()
    out.local().start()

    row = lax.broadcasted_iota(jnp.int32, (256, 256), 0)
    lane = lax.broadcasted_iota(jnp.int32, (256, 256), 1)
    masked = jnp.max(jnp.where(remask_ref[...] == row, 1.0, 0.0), axis=1, keepdims=True)
    ids_col = jnp.sum(
        jnp.where(row == lane, ids_ref[...].astype(F32), 0.0), axis=1, keepdims=True
    )
    weight[...] = jnp.broadcast_to(masked, (256, 128))
    ids_col = jnp.where(masked > 0.5, -1.0, ids_col)
    entry = lax.broadcasted_iota(jnp.int32, (256, 512), 1)
    mask_row = mask_embed_ref[...].astype(F32).reshape(1, 1024)

    def looked_up(half):
        onehot = jnp.where((entry + half * 512).astype(F32) == ids_col, 1.0, 0.0).astype(BF)
        rows = table[pl.ds(pl.multiple_of(half * 512, 512), 512)]
        return jnp.dot(onehot, rows, preferred_element_type=F32)

    load_pos.wait()
    for k in range(4):
        block = slice(k * 64, k * 64 + 64)
        hidden[block] = pos[block].astype(F32) + jnp.where(masked[block] > 0.5, mask_row, 0.0)
    tab.local().wait()
    out.local().wait()
    pl.semaphore_wait(barrier, len(peers))
    tab.start_z()
    tab.start_own_quarter()
    out.start_z()
    tab.start_y()
    arrived(table.at[pl.ds(0, 256)], tab.dsem.at[0])
    hidden[...] += looked_up(zh)
    tab.start_x()
    out.start_x_first()
    tab.finish_x()
    out.start_y_second()
    out.start_own_quarter()
    load_qkv.wait()
    arrived(table.at[pl.ds(0, 256)], tab.dsem.at[1])
    hidden[...] += looked_up(1 - zh)
    gain_in = gain_in_ref[...]
    for k in range(4):
        block = slice(k * 64, k * 64 + 64)
        normed[block] = norm_rows(hidden[block], gain_in).astype(BF)
    low = lax.broadcasted_iota(jnp.int32, (256, 128), 1) < 64
    n_all = normed[...]
    keys = jnp.dot(n_all, wqkv[1], preferred_element_type=F32)
    values = jnp.dot(n_all, wqkv[2], preferred_element_type=F32)
    for g in range(2):
        kg, vg = keys[:, g * 128 : g * 128 + 128], values[:, g * 128 : g * 128 + 128]
        kv_out[2 * g] = jnp.where(low, kg, pltpu.roll(vg, 64, 1)).astype(BF)
        kv_out[2 * g + 1] = jnp.where(low, pltpu.roll(kg, 64, 1), vg).astype(BF)
    query = jnp.dot(n_all, wqkv[0], preferred_element_type=F32)
    low_half = low[:128]
    for g in range(2):
        qa, qb = query[:128, g * 128 : g * 128 + 128], query[128:, g * 128 : g * 128 + 128]
        q_out[2 * g] = jnp.where(low_half, qa, pltpu.roll(qb, 64, 1)).astype(BF)
        q_out[2 * g + 1] = jnp.where(low_half, pltpu.roll(qa, 64, 1), qb).astype(BF)
    def pass_on(block, s):
        for dx in (1, 3, 2):
            slot = (0, 1, 3, 2)[dx]
            remote(block, kv.at[s, slot], b_send.at[0], b_recv.at[s, slot], at(0, 0, dx, 0, 0)).start()

    pass_on(kv_out.at[zl], 0)
    for dz in (1, 3, 2):
        head = lax.rem(zl + dz, 4)
        remote(
            q_out.at[head], q_in.at[4 - dz], a_send.at[1], q_recv.at[4 - dz], at(0, dz, 0, 0, 0)
        ).start()
    for dz in (3, 1, 2):
        head = lax.rem(zl + dz, 4)
        remote(
            kv_out.at[head], kv.at[4 - dz, 0], a_send.at[0], a_recv.at[4 - dz], at(0, dz, 0, 0, 0)
        ).start()
    kv[0, 0] = kv_out[zl]

    def unpack(k, packed):
        packed = packed.astype(F32)
        qpad[k, :128] = jnp.where(low_half, packed, 0.0).astype(BF)
        qpad[k, 128:] = jnp.where(low_half, pltpu.roll(packed, 64, 1), 0.0).astype(BF)

    unpack(0, q_out[zl])
    low64 = low[:64]
    head_here = mp * 4 + zl

    def ready(s, b):
        if s == 0:
            if b == 0:
                for slot in (1, 2, 3):
                    arrived(kv.at[0, slot], b_recv.at[0, slot])
            else:
                arrived(q_in.at[b], q_recv.at[b])
                unpack(b, q_in[b])
        elif b == 0:
            for slot in (1, 2, 3):
                arrived(kv.at[s, slot], b_recv.at[s, slot])

    def score(s, b):
        return lax.dot_general(
            qpad[b], kv[s].reshape(1024, 128), (((1,), (1,)), ((), ())), preferred_element_type=F32
        )

    def absorb(s, b, scores):
        rows = kv[s].reshape(1024, 128)
        top = jnp.max(scores, axis=1, keepdims=True)
        if s == 0:
            w = jnp.exp2(scores * SCALE - top * SCALE)
            high[b] = jnp.broadcast_to(top, (256, 128))
            total[b] = jnp.broadcast_to(jnp.sum(w, axis=1, keepdims=True), (256, 128))
            summed[b] = jnp.dot(w.astype(BF), rows, preferred_element_type=F32)
            return
        before = high[b]
        now = jnp.maximum(before, top)
        fade = jnp.exp2((before - now) * SCALE)
        w = jnp.exp2(scores * SCALE - now[:, :1] * SCALE)
        sums = total[b] * fade + jnp.sum(w, axis=1, keepdims=True)
        acc = summed[b] * fade + jnp.dot(w.astype(BF), rows, preferred_element_type=F32)
        if s != 2:
            high[b], total[b], summed[b] = now, sums, acc
            return
        rows = acc / sums
        for half in range(2):
            top_rows = rows[half * 128 : half * 128 + 64]
            low_rows = rows[half * 128 + 64 : half * 128 + 128]
            o_out[b, half] = jnp.where(low64, pltpu.roll(top_rows, 64, 1), low_rows).astype(BF)

    def send_context(b):
        for dh in (1, 0):
            for dc in (0, 1):
                if b == 0 and dh == 0 and dc == 0:
                    continue
                half = lax.rem(core + dc, 2)
                remote(
                    o_out.at[b, half], ctx.at[head_here], c_send.at[0], c_recv.at[0], at(0, b, 0, dh, dc)
                ).start()

    steps = [(s, b) for s in (0, 1, 3, 2) for b in (0, 1, 3, 2)]
    ready(0, 0)
    scores = score(0, 0)
    for i, (s, b) in enumerate(steps):
        for arriving in {(0, 2): (1, 3), (1, 1): (2,)}.get((s, b), ()):
            arrived(kv.at[arriving, 0], a_recv.at[arriving])
            pass_on(kv.at[arriving, 0], arriving)
        if i + 1 < len(steps):
            ready(*steps[i + 1])
            following = score(*steps[i + 1])
        absorb(s, b, scores)
        if s == 2:
            send_context(b)
        scores = following
    out.finish_y_second()
    ctx[head_here] = o_out[0, core]
    out.wait_all()
    arrived(ctx.at[pl.ds(0, 15)], c_recv.at[0])
    pieces = []
    for g in range(8):
        a, b = ctx[2 * g].astype(F32), ctx[2 * g + 1].astype(F32)
        pieces.append(
            jnp.concatenate(
                [
                    jnp.where(low64, a, pltpu.roll(b, 64, 1)),
                    jnp.where(low64, pltpu.roll(a, 64, 1), b),
                ],
                axis=0,
            ).astype(BF)
        )
    context = jnp.concatenate(pieces, axis=1)
    mine = pl.ds(pl.multiple_of(core * 128, 128), 128)
    h = hidden[mine] + jnp.dot(context, wout[...], preferred_element_type=F32)
    final[mine] = norm_rows(h, gain_out_ref[...]).astype(BF)
    send_final = remote(final.at[mine], final.at[mine], f_send.at[0], f_recv.at[0], at(0, 0, 0, 0, 1))
    send_final.start()

    def finish(block):
        rows = final[block]
        tops = []
        for q in range(4):
            part = lax.dot_general(
                rows, table[q * 256 : q * 256 + 256], (((1,), (1,)), ((), ())), preferred_element_type=F32
            )
            logits[q, block] = part
            tops.append(jnp.max(part, axis=1, keepdims=True))
        top = jnp.maximum(jnp.maximum(tops[0], tops[1]), jnp.maximum(tops[2], tops[3]))
        sums = jnp.zeros_like(top)
        for q in range(4):
            sums = sums + jnp.sum(jnp.exp(logits[q, block] - top), axis=1, keepdims=True)
        lse = top + jnp.log(sums)
        logp_ref[0, block] = (logits[mp, block] - lse).astype(BF)
        conf = jnp.exp(top - lse)
        high[0, block] = jnp.broadcast_to(conf, (128, 128))
        return conf

    conf = finish(mine)
    w = weight[mine][:, :1]
    lane8 = lax.broadcasted_iota(jnp.int32, (8, 128), 1)
    conf_sum = jnp.sum(conf * w, axis=0, keepdims=True)
    count = jnp.sum(w, axis=0, keepdims=True)
    tile = jnp.where(lane8 == 0, conf_sum, jnp.where(lane8 == 1, count, 0.0))
    place = frame * 2 + core
    stat_out[...] = tile
    stat_in[place] = tile
    for dz in (2, 3, 1, 0):
        for dx in (2, 3, 1, 0):
            for dc in range(2):
                if dz or dx or dc:
                    remote(
                        stat_out, stat_in.at[place], s_send.at[0], s_recv.at[0], at(0, dz, dx, 0, dc)
                    ).start()
    other = pl.ds(pl.multiple_of((1 - core) * 128, 128), 128)
    arrived(final.at[other], f_recv.at[0])
    finish(other)
    conf_ref[...] = jnp.sum(jnp.where(row == lane, high[0][:, :1], 0.0), axis=0, keepdims=True)
    tab.wait_sent()
    out.wait_sent_x_first()
    left(kv_out.at[pl.ds(0, 3)], a_send.at[0])
    left(q_out.at[pl.ds(0, 3)], a_send.at[1])
    left(kv.at[pl.ds(0, 3)], b_send.at[0])
    left(ctx.at[pl.ds(0, 15)], c_send.at[0])
    send_final.wait_send()
    arrived(stat_in.at[pl.ds(0, 31)], s_recv.at[0])
    left(stat_in.at[pl.ds(0, 31)], s_send.at[0])
    sums = stat_in[0]
    for k in range(1, 32):
        sums = sums + stat_in[k]
    sums = sums[:1]
    lane1 = lane8[:1]
    all_conf = jnp.sum(jnp.where(lane1 == 0, sums, 0.0), axis=1, keepdims=True)
    all_count = jnp.sum(jnp.where(lane1 == 1, sums, 0.0), axis=1, keepdims=True)
    stats_ref[...] = jnp.where(lane1 == 0, all_conf / all_count, jnp.log(all_count / 4096.0))


def write_out(logp, conf, stats, logp_out, conf_out, stats_out):
    logp_out[...] = logp[...]
    conf_out[...] = conf[...]
    stats_out[...] = stats[:, :2]


def body(token_ids, remask, position_embed, mask_embed, table, gain_in, gain_out, w_qkv, w_out):
    vmem = pl.BlockSpec(memory_space=pltpu.VMEM)
    hbm = pl.BlockSpec(memory_space=pl.ANY)
    dma = pltpu.SemaphoreType.DMA
    spread_sems = [dma((5,)), dma, dma((8,)), dma((4,)), dma((2,))]
    log_probs, confidence, stats = pl.pallas_call(
        kernel,
        out_shape=(
            jax.ShapeDtypeStruct((1, 256, 256), BF),
            jax.ShapeDtypeStruct((1, 256), F32),
            jax.ShapeDtypeStruct((1, 128), F32),
        ),
        in_specs=[vmem] * 5 + [hbm] * 4,
        out_specs=(vmem, vmem, vmem),
        scratch_shapes=[
            pltpu.VMEM((1024, 1024), BF),
            pltpu.VMEM((1024, 1024), BF),
            pltpu.VMEM((3, 1024, 256), BF),
            pltpu.VMEM((256, 1024), BF),
            pltpu.VMEM((256, 1024), F32),
            pltpu.VMEM((256, 1024), BF),
            pltpu.VMEM((4, 256, 128), BF),
            pltpu.VMEM((4, 128, 128), BF),
            pltpu.VMEM((4, 4, 256, 128), BF),
            pltpu.VMEM((4, 128, 128), BF),
            pltpu.VMEM((4, 256, 128), BF),
            pltpu.VMEM((4, 256, 128), F32),
            pltpu.VMEM((4, 256, 128), F32),
            pltpu.VMEM((4, 256, 128), F32),
            pltpu.VMEM((4, 2, 64, 128), BF),
            pltpu.VMEM((16, 64, 128), BF),
            pltpu.VMEM((256, 1024), BF),
            pltpu.VMEM((4, 256, 256), F32),
            pltpu.VMEM((256, 128), F32),
            pltpu.VMEM((8, 128), F32),
            pltpu.VMEM((32, 8, 128), F32),
            dma((2,)),
            *spread_sems,
            *spread_sems,
            dma((2,)),
            dma((4,)),
            dma((4,)),
            dma((1,)),
            dma((4, 4)),
            dma((1,)),
            dma((1,)),
            dma((1,)),
            dma((1,)),
            dma((1,)),
            dma((1,)),
        ],
        compiler_params=pltpu.CompilerParams(
            collective_id=0, has_side_effects=True, vmem_limit_bytes=60 * 1024 * 1024
        ),
        name="predict",
    )(
        token_ids,
        remask,
        mask_embed,
        gain_in.reshape(1, -1),
        gain_out.reshape(1, -1),
        table,
        w_qkv,
        w_out,
        position_embed,
    )
    log_probs, confidence, stats = pl.pallas_call(
        write_out,
        out_shape=(
            jax.ShapeDtypeStruct((1, 256, 256), BF),
            jax.ShapeDtypeStruct((1, 256), F32),
            jax.ShapeDtypeStruct((1, 2), F32),
        ),
        in_specs=[vmem] * 3,
        out_specs=(vmem, vmem, vmem),
        name="write_out",
    )(log_probs, confidence, stats)
    return log_probs, confidence, stats.reshape(2)


def solution(mesh):
    finer = Mesh(mesh.devices.reshape(8, 4, 4, 2, 2), AXES)
    frames = ("clip", "zl", "x")
    tm = ("zl", "x")
    mp = ("zh", "core")
    in_specs = (
        P(frames, None),
        P(frames, None),
        P(tm, None, None),
        P(),
        P(mp, None),
        P(),
        P(),
        P(None, None, mp),
        P(mp, None),
    )
    out_specs = (P(frames, None, mp), P(frames, None), P("clip"))
    return jax.shard_map(body, mesh=finer, in_specs=in_specs, out_specs=out_specs, check_vma=False)
```

```python
import math

import jax
import jax.numpy as jnp
from jax import lax
from jax.experimental import pallas as pl
from jax.experimental.pallas import tpu as pltpu
from jax.sharding import Mesh
from jax.sharding import PartitionSpec as P

HEAD_DIM = 64
MESH = pl.DeviceIdType.MESH
AXES = ("clip", "zl", "x", "zh", "core")
BF = jnp.bfloat16
F32 = jnp.float32
SCALE = HEAD_DIM**-0.5 * math.log2(math.e)


def coords():
    return [lax.axis_index(name) for name in AXES]


def at(y, zl, x, zh, core):
    mine = coords()
    sizes = (8, 4, 4, 2, 2)
    return tuple(
        lax.rem(mine[k] + step + sizes[k], sizes[k]) if step else mine[k]
        for k, step in enumerate((y, zl, x, zh, core))
    )


def mirror():
    y, zl, x, zh, core = coords()
    return (y, 3 - zl, x, 1 - zh, core)


def remote(src, dst, send, recv, device):
    return pltpu.make_async_remote_copy(
        src_ref=src, dst_ref=dst, send_sem=send, recv_sem=recv, device_id=device, device_id_type=MESH
    )


def arrived(ref, sem):
    remote(ref, ref, sem, sem, at(0, 0, 0, 0, 1)).wait_recv()


def left(ref, sem):
    remote(ref, ref, sem, sem, at(0, 0, 0, 0, 1)).wait_send()


def norm_rows(h, gain):
    center = h - jnp.mean(h, axis=-1, keepdims=True)
    spread = jnp.mean(center * center, axis=-1, keepdims=True)
    return center * lax.rsqrt(spread + 1e-05) * gain


class Spread:
    def __init__(self, hbm, full, first, ssem, zsem, y1sem, x1sem, y2sem, x2sem, dsem):
        self.hbm, self.full, self.first, self.ssem, self.zsem, self.dsem = hbm, full, first, ssem, zsem, dsem
        self.y1, self.x1, self.y2, self.x2 = y1sem, x1sem, y2sem, x2sem
        y, zl, x, zh, core = coords()
        self.yq, self.x = lax.rem(y, 4), x
        self.own = zh * 2 + core
        self.got = (1 - zh) * 2 + core

    def quarter(self, k):
        return pl.ds(pl.multiple_of(k * 256, 256), 256)

    def rows(self, quarter, x):
        return pl.ds(pl.multiple_of(quarter * 256 + x * 64, 64), 64)

    def cols(self, yq, half):
        return pl.ds(pl.multiple_of(half * 512 + yq * 128, 128), 128)

    def piece(self, x, yq, half):
        return self.full.at[self.rows(self.got, x), self.cols(yq, half)]

    def strip(self, yq, half):
        return self.full.at[self.quarter(self.got), self.cols(yq, half)]

    def block(self, x):
        return self.full.at[self.rows(self.got, x), pl.ds(0, 512)]

    def y_of(self, dy):
        return lax.rem(self.yq - dy + 8, 4)

    def x_of(self, dx):
        return lax.rem(self.x - dx + 4, 4)

    def local(self):
        return pltpu.make_async_copy(self.hbm, self.full.at[self.quarter(self.own)], self.ssem.at[4])

    def fetch(self, half):
        rows = pl.ds(pl.multiple_of(self.x * 64, 64), 64)
        return pltpu.make_async_copy(
            self.hbm.at[rows, self.cols(self.yq, half)], self.first.at[half], self.ssem.at[5 + half]
        )

    def start_z(self):
        for half in range(2):
            piece = self.full.at[self.rows(self.own, self.x), self.cols(self.yq, half)]
            remote(self.first.at[half], piece, self.ssem.at[0], self.zsem.at[half], mirror()).start()

    def start_own_quarter(self):
        self.hand_over(self.full.at[self.quarter(self.own)], 0)

    def hand_over(self, ref, k):
        remote(ref, ref, self.ssem.at[3], self.dsem.at[k], at(0, 0, 0, 0, 1)).start()

    def along_y(self, ref, sem, recv):
        for dy in (2, 1, 7):
            remote(ref, ref, self.ssem.at[sem], recv.at[dy], at(dy, 0, 0, 0, 0)).start()

    def along_x(self, ref, sem, recv):
        for dx in (2, 1, 3):
            remote(ref, ref, self.ssem.at[sem], recv.at[dx], at(0, 0, dx, 0, 0)).start()

    def begin(self):
        first, second = self.piece(self.x, self.yq, 0), self.piece(self.x, self.yq, 1)
        arrived(first, self.zsem.at[0])
        self.along_y(first, 1, self.y1)
        arrived(second, self.zsem.at[1])
        self.along_x(second, 1, self.x1)
        self.along_x(first, 2, self.x2)
        self.along_y(second, 2, self.y2)

    def forward(self):
        for dy, dx in ((1, 1), (7, 3), (2, 2)):
            first = self.piece(self.x, self.y_of(dy), 0)
            arrived(first, self.y1.at[dy])
            self.along_x(first, 2, self.x2)
            second = self.piece(self.x_of(dx), self.yq, 1)
            arrived(second, self.x1.at[dx])
            self.along_y(second, 2, self.y2)
        self.hand_over(self.block(self.x), 1)
        self.hand_over(self.strip(self.yq, 1), 1)

    def finish(self):
        for dy, dx in ((1, 1), (7, 3), (2, 2)):
            block = self.block(self.x_of(dx))
            arrived(block, self.x2.at[dx])
            self.hand_over(block, 1)
            strip = self.strip(self.y_of(dy), 1)
            arrived(strip, self.y2.at[dy])
            self.hand_over(strip, 1)

    def wait_sent(self):
        left(self.full.at[pl.ds(0, 64), pl.ds(0, 256)], self.ssem.at[0])
        left(self.full.at[pl.ds(0, 64), pl.ds(0, 768)], self.ssem.at[1])
        left(self.full.at[pl.ds(0, 192)], self.ssem.at[2])
        left(self.full.at[pl.ds(0, 512)], self.ssem.at[3])

    def begin_slow(self):
        for half in range(2):
            piece = self.piece(self.x, self.yq, half)
            arrived(piece, self.zsem.at[half])
            self.along_x(piece, 1, self.x1)

    def forward_slow(self):
        for dx in (1, 3, 2):
            arrived(self.full.at[self.rows(self.got, self.x_of(dx)), pl.ds(0, 256)], self.x1.at[dx])
        for half in range(2):
            self.along_y(self.strip(self.yq, half), 2, self.y2)

    def finish_slow(self):
        for dy in (1, 7, 2):
            arrived(self.full.at[self.quarter(self.got), pl.ds(0, 256)], self.y2.at[dy])
        self.hand_over(self.full.at[self.quarter(self.got)], 1)

    def wait_sent_slow(self):
        left(self.full.at[pl.ds(0, 64), pl.ds(0, 256)], self.ssem.at[0])
        left(self.full.at[pl.ds(0, 64), pl.ds(0, 768)], self.ssem.at[1])
        left(self.full.at[pl.ds(0, 256), pl.ds(0, 768)], self.ssem.at[2])
        left(self.full.at[pl.ds(0, 512)], self.ssem.at[3])

    def wait_all(self):
        quarter = self.full.at[pl.ds(0, 256)]
        arrived(quarter, self.dsem.at[0])
        arrived(quarter, self.dsem.at[1])


def kernel(
    ids_hbm, remask_hbm, mask_hbm, gain_in_hbm, gain_out_hbm, table_hbm, wqkv_hbm, wout_hbm, pos_hbm,
    logp_hbm, conf_hbm, stats_hbm,
    ids_ref, remask_ref, mask_embed_ref, gain_in_ref, gain_out_ref, logp_ref, conf_ref, stats_ref,
    table_first, wout_first, table, wout, wqkv, pos, hidden, normed, kv_out, q_out, kv, q_in, qpad, high, total, summed, o_out, ctx,
    final, logits, weight, stat_out, stat_in,
    local_sem, small_sem, put_sem,
    t_s, t_z, t_y1, t_x1, t_y2, t_x2, t_d, w_s, w_z, w_y1, w_x1, w_y2, w_x2, w_d,
    a_send, a_recv, q_recv, b_send, b_recv,
    c_send, c_recv, f_send, f_recv, s_send, s_recv,
):
    y, zl, x, zh, core = coords()
    mp = zh * 2 + core
    frame = zl * 4 + x
    pair_z = (zl, zl + 1 - 2 * lax.rem(zl, 2), lax.rem(zl + 2, 4), 3 - zl)
    tab = Spread(table_hbm, table, table_first, t_s, t_z, t_y1, t_x1, t_y2, t_x2, t_d)
    out = Spread(wout_hbm, wout, wout_first, w_s, w_z, w_y1, w_x1, w_y2, w_x2, w_d)
    load_pos = pltpu.make_async_copy(pos_hbm.at[0], pos, local_sem.at[0])
    load_qkv = pltpu.make_async_copy(wqkv_hbm, wqkv, local_sem.at[1])

    small = [
        pltpu.make_async_copy(src, dst, small_sem.at[k])
        for k, (src, dst) in enumerate(
            (
                (ids_hbm, ids_ref),
                (remask_hbm, remask_ref),
                (mask_hbm, mask_embed_ref),
                (gain_in_hbm, gain_in_ref),
                (gain_out_hbm, gain_out_ref),
            )
        )
    ]
    for half in range(2):
        tab.fetch(half).start()
    barrier = pltpu.get_barrier_semaphore()
    peers = []
    for k in range(1, 16):
        place = lax.rem(zh * 8 + zl * 2 + core + k, 16)
        peers.append((y, lax.rem(place // 2, 4), x, place // 8, lax.rem(place, 2)))
    peers += [at(k, 0, 0, 0, 0) for k in (1, 2, 6, 7)]
    peers += [at(0, dz, dx, 0, dc) for dx in range(1, 4) for dz in range(4) for dc in range(2)]
    for peer in peers:
        pl.semaphore_signal(barrier, inc=1, device_id=peer, device_id_type=MESH)
    tab.local().start()
    for copy in small:
        copy.start()
    load_pos.start()
    out.local().start()
    for half in range(2):
        out.fetch(half).start()
    load_qkv.start()
    for half in range(2):
        tab.fetch(half).wait()
    pl.semaphore_wait(barrier, len(peers))
    tab.start_z()
    tab.local().wait()
    tab.start_own_quarter()
    for copy in small:
        copy.wait()
    row = lax.broadcasted_iota(jnp.int32, (256, 256), 0)
    lane = lax.broadcasted_iota(jnp.int32, (256, 256), 1)
    masked = jnp.max(jnp.where(remask_ref[...] == row, 1.0, 0.0), axis=1, keepdims=True)
    ids_col = jnp.sum(
        jnp.where(row == lane, ids_ref[...].astype(F32), 0.0), axis=1, keepdims=True
    )
    weight[...] = jnp.broadcast_to(masked, (256, 128))
    ids_col = jnp.where(masked > 0.5, -1.0, ids_col)
    entry = lax.broadcasted_iota(jnp.int32, (256, 512), 1)
    mask_row = mask_embed_ref[...].astype(F32).reshape(1, 1024)

    def looked_up(half):
        onehot = jnp.where((entry + half * 512).astype(F32) == ids_col, 1.0, 0.0).astype(BF)
        rows = table[pl.ds(pl.multiple_of(half * 512, 512), 512)]
        return jnp.dot(onehot, rows, preferred_element_type=F32)

    load_pos.wait()
    for k in range(4):
        block = slice(k * 64, k * 64 + 64)
        hidden[block] = pos[block].astype(F32) + jnp.where(masked[block] > 0.5, mask_row, 0.0)
    tab.begin()
    for half in range(2):
        out.fetch(half).wait()
    out.start_z()
    arrived(table.at[pl.ds(0, 256)], tab.dsem.at[0])
    hidden[...] += looked_up(zh)
    tab.forward()
    out.begin_slow()
    tab.finish()
    out.forward_slow()
    out.local().wait()
    out.start_own_quarter()
    load_qkv.wait()
    arrived(table.at[pl.ds(0, 256)], tab.dsem.at[1])
    hidden[...] += looked_up(1 - zh)
    gain_in = gain_in_ref[...]
    for k in range(4):
        block = slice(k * 64, k * 64 + 64)
        normed[block] = norm_rows(hidden[block], gain_in).astype(BF)
    low = lax.broadcasted_iota(jnp.int32, (256, 128), 1) < 64
    n_all = normed[...]
    keys = jnp.dot(n_all, wqkv[1], preferred_element_type=F32)
    values = jnp.dot(n_all, wqkv[2], preferred_element_type=F32)
    for g in range(2):
        kg, vg = keys[:, g * 128 : g * 128 + 128], values[:, g * 128 : g * 128 + 128]
        kv_out[2 * g] = jnp.where(low, kg, pltpu.roll(vg, 64, 1)).astype(BF)
        kv_out[2 * g + 1] = jnp.where(low, pltpu.roll(kg, 64, 1), vg).astype(BF)
    query = jnp.dot(n_all, wqkv[0], preferred_element_type=F32)
    low_half = low[:128]
    for g in range(2):
        qa, qb = query[:128, g * 128 : g * 128 + 128], query[128:, g * 128 : g * 128 + 128]
        q_out[2 * g] = jnp.where(low_half, qa, pltpu.roll(qb, 64, 1)).astype(BF)
        q_out[2 * g + 1] = jnp.where(low_half, pltpu.roll(qa, 64, 1), qb).astype(BF)
    def pass_on(block, s):
        for dx in (1, 3, 2):
            slot = (0, 1, 3, 2)[dx]
            remote(block, kv.at[s, slot], b_send.at[0], b_recv.at[s, slot], at(0, 0, dx, 0, 0)).start()

    pass_on(kv_out.at[zl], 0)
    def send_keys(d):
        remote(
            kv_out.at[pair_z[d]], kv.at[d, 0], a_send.at[0], a_recv.at[d], (y, pair_z[d], x, zh, core)
        ).start()

    def send_query(d):
        remote(
            q_out.at[pair_z[d]], q_in.at[d], a_send.at[1], q_recv.at[d], (y, pair_z[d], x, zh, core)
        ).start()

    send_keys(2)
    send_keys(1)
    send_query(1)
    send_query(2)
    send_keys(3)
    send_query(3)
    kv[0, 0] = kv_out[zl]

    def unpack(k, packed):
        packed = packed.astype(F32)
        qpad[k, :128] = jnp.where(low_half, packed, 0.0).astype(BF)
        qpad[k, 128:] = jnp.where(low_half, pltpu.roll(packed, 64, 1), 0.0).astype(BF)

    unpack(0, q_out[zl])
    low64 = low[:64]
    head_here = mp * 4 + zl

    def take(s):
        arrived(kv.at[s, 0], a_recv.at[s])
        pass_on(kv.at[s, 0], s)

    held = set()

    def ready(s, b):
        if b and (b, "q") not in held:
            arrived(q_in.at[b], q_recv.at[b])
            unpack(b, q_in[b])
            held.add((b, "q"))
        if s not in held:
            for slot in (1, 2, 3):
                arrived(kv.at[s, slot], b_recv.at[s, slot])
            held.add(s)

    def score(s, b):
        return lax.dot_general(
            qpad[b], kv[s].reshape(1024, 128), (((1,), (1,)), ((), ())), preferred_element_type=F32
        )

    def absorb(s, b, scores):
        rows = kv[s].reshape(1024, 128)
        top = jnp.max(scores, axis=1, keepdims=True)
        if s == 0:
            w = jnp.exp2(scores * SCALE - top * SCALE)
            high[b] = jnp.broadcast_to(top, (256, 128))
            total[b] = jnp.broadcast_to(jnp.sum(w, axis=1, keepdims=True), (256, 128))
            summed[b] = jnp.dot(w.astype(BF), rows, preferred_element_type=F32)
            return
        before = high[b]
        now = jnp.maximum(before, top)
        fade = jnp.exp2((before - now) * SCALE)
        w = jnp.exp2(scores * SCALE - now[:, :1] * SCALE)
        sums = total[b] * fade + jnp.sum(w, axis=1, keepdims=True)
        acc = summed[b] * fade + jnp.dot(w.astype(BF), rows, preferred_element_type=F32)
        if s != 3:
            high[b], total[b], summed[b] = now, sums, acc
            return
        rows = acc / sums
        for half in range(2):
            top_rows = rows[half * 128 : half * 128 + 64]
            low_rows = rows[half * 128 + 64 : half * 128 + 128]
            o_out[b, half] = jnp.where(low64, pltpu.roll(top_rows, 64, 1), low_rows).astype(BF)

    def send_context(b):
        for dh in (1, 0):
            for dc in (0, 1):
                if b == 0 and dh == 0 and dc == 0:
                    continue
                half = lax.rem(core + dc, 2)
                there = (y, pair_z[b], x, lax.rem(zh + dh, 2), half)
                remote(
                    o_out.at[b, half], ctx.at[head_here], c_send.at[0], c_recv.at[0], there
                ).start()

    steps = [(s, b) for s in (0, 2) for b in (0, 1, 2)] + [(0, 3), (2, 3)]
    steps += [(s, b) for s in (1, 3) for b in (2, 3, 1, 0)]
    take(2)
    take(1)
    ready(0, 0)
    scores = score(0, 0)
    for i, (s, b) in enumerate(steps):
        if i + 1 < len(steps):
            if steps[i + 1] == (2, 0):
                take(3)
            ready(*steps[i + 1])
            following = score(*steps[i + 1])
        absorb(s, b, scores)
        if s == 3:
            send_context(b)
        scores = following
    out.finish_slow()
    ctx[head_here] = o_out[0, core]
    out.wait_all()
    arrived(ctx.at[pl.ds(0, 15)], c_recv.at[0])
    pieces = []
    for g in range(8):
        a, b = ctx[2 * g].astype(F32), ctx[2 * g + 1].astype(F32)
        pieces.append(
            jnp.concatenate(
                [
                    jnp.where(low64, a, pltpu.roll(b, 64, 1)),
                    jnp.where(low64, pltpu.roll(a, 64, 1), b),
                ],
                axis=0,
            ).astype(BF)
        )
    context = jnp.concatenate(pieces, axis=1)
    mine = pl.ds(pl.multiple_of(core * 128, 128), 128)
    h = hidden[mine] + jnp.dot(context, wout[...], preferred_element_type=F32)
    final[mine] = norm_rows(h, gain_out_ref[...]).astype(BF)
    send_final = remote(final.at[mine], final.at[mine], f_send.at[0], f_recv.at[0], at(0, 0, 0, 0, 1))
    send_final.start()

    def finish(block):
        rows = final[block]
        tops = []
        for q in range(4):
            part = lax.dot_general(
                rows, table[q * 256 : q * 256 + 256], (((1,), (1,)), ((), ())), preferred_element_type=F32
            )
            logits[q, block] = part
            tops.append(jnp.max(part, axis=1, keepdims=True))
        top = jnp.maximum(jnp.maximum(tops[0], tops[1]), jnp.maximum(tops[2], tops[3]))
        sums = jnp.zeros_like(top)
        for q in range(4):
            sums = sums + jnp.sum(jnp.exp(logits[q, block] - top), axis=1, keepdims=True)
        lse = top + jnp.log(sums)
        logp_ref[block] = (logits[mp, block] - lse).astype(BF)
        conf = jnp.exp(top - lse)
        high[0, block] = jnp.broadcast_to(conf, (128, 128))
        return conf

    conf = finish(mine)
    w = weight[mine][:, :1]
    lane8 = lax.broadcasted_iota(jnp.int32, (8, 128), 1)
    conf_sum = jnp.sum(conf * w, axis=0, keepdims=True)
    count = jnp.sum(w, axis=0, keepdims=True)
    tile = jnp.where(lane8 == 0, conf_sum, jnp.where(lane8 == 1, count, 0.0))
    place = frame * 2 + core
    stat_out[...] = tile
    stat_in[place] = tile
    for dz in (2, 3, 1, 0):
        for dx in (2, 3, 1, 0):
            for dc in range(2):
                if dz or dx or dc:
                    remote(
                        stat_out, stat_in.at[place], s_send.at[0], s_recv.at[0], at(0, dz, dx, 0, dc)
                    ).start()
    other = pl.ds(pl.multiple_of((1 - core) * 128, 128), 128)
    arrived(final.at[other], f_recv.at[0])
    finish(other)
    conf_ref[...] = jnp.sum(jnp.where(row == lane, high[0][:, :1], 0.0), axis=0, keepdims=True)
    put = [
        pltpu.make_async_copy(logp_ref, logp_hbm.at[0], put_sem.at[0]),
        pltpu.make_async_copy(conf_ref, conf_hbm, put_sem.at[1]),
        pltpu.make_async_copy(stats_ref, stats_hbm, put_sem.at[2]),
    ]
    put[0].start()
    put[1].start()
    tab.wait_sent()
    out.wait_sent_slow()
    left(kv_out.at[pl.ds(0, 3)], a_send.at[0])
    left(q_out.at[pl.ds(0, 3)], a_send.at[1])
    left(kv.at[pl.ds(0, 3)], b_send.at[0])
    left(ctx.at[pl.ds(0, 15)], c_send.at[0])
    send_final.wait_send()
    arrived(stat_in.at[pl.ds(0, 31)], s_recv.at[0])
    left(stat_in.at[pl.ds(0, 31)], s_send.at[0])
    sums = stat_in[0]
    for k in range(1, 32):
        sums = sums + stat_in[k]
    sums = sums[:1]
    lane1 = lane8[:1]
    all_conf = jnp.sum(jnp.where(lane1 == 0, sums, 0.0), axis=1, keepdims=True)
    all_count = jnp.sum(jnp.where(lane1 == 1, sums, 0.0), axis=1, keepdims=True)
    stats_ref[...] = jnp.where(lane1 == 0, all_conf / all_count, jnp.log(all_count / 4096.0))
    put[2].start()
    for copy in put:
        copy.wait()


def write_out(logp, conf, stats, logp_out, conf_out, stats_out):
    logp_out[...] = logp[...]
    conf_out[...] = conf[...]
    stats_out[...] = stats[:, :2]


def body(token_ids, remask, position_embed, mask_embed, table, gain_in, gain_out, w_qkv, w_out):
    vmem = pl.BlockSpec(memory_space=pltpu.VMEM)
    hbm = pl.BlockSpec(memory_space=pl.ANY)
    dma = pltpu.SemaphoreType.DMA
    spread_sems = [dma((7,)), dma((2,)), dma((8,)), dma((4,)), dma((8,)), dma((4,)), dma((2,))]
    log_probs, confidence, stats = pl.pallas_call(
        kernel,
        out_shape=(
            jax.ShapeDtypeStruct((1, 256, 256), BF),
            jax.ShapeDtypeStruct((1, 256), F32),
            jax.ShapeDtypeStruct((1, 128), F32),
        ),
        in_specs=[hbm] * 9,
        out_specs=(hbm, hbm, hbm),
        scratch_shapes=[
            pltpu.VMEM((1, 256), jnp.int32),
            pltpu.VMEM((1, 256), jnp.int32),
            pltpu.VMEM((1024,), BF),
            pltpu.VMEM((1, 1024), F32),
            pltpu.VMEM((1, 1024), F32),
            pltpu.VMEM((256, 256), BF),
            pltpu.VMEM((1, 256), F32),
            pltpu.VMEM((1, 128), F32),
            pltpu.VMEM((2, 64, 128), BF),
            pltpu.VMEM((2, 64, 128), BF),
            pltpu.VMEM((1024, 1024), BF),
            pltpu.VMEM((1024, 1024), BF),
            pltpu.VMEM((3, 1024, 256), BF),
            pltpu.VMEM((256, 1024), BF),
            pltpu.VMEM((256, 1024), F32),
            pltpu.VMEM((256, 1024), BF),
            pltpu.VMEM((4, 256, 128), BF),
            pltpu.VMEM((4, 128, 128), BF),
            pltpu.VMEM((4, 4, 256, 128), BF),
            pltpu.VMEM((4, 128, 128), BF),
            pltpu.VMEM((4, 256, 128), BF),
            pltpu.VMEM((4, 256, 128), F32),
            pltpu.VMEM((4, 256, 128), F32),
            pltpu.VMEM((4, 256, 128), F32),
            pltpu.VMEM((4, 2, 64, 128), BF),
            pltpu.VMEM((16, 64, 128), BF),
            pltpu.VMEM((256, 1024), BF),
            pltpu.VMEM((4, 256, 256), F32),
            pltpu.VMEM((256, 128), F32),
            pltpu.VMEM((8, 128), F32),
            pltpu.VMEM((32, 8, 128), F32),
            dma((2,)),
            dma((5,)),
            dma((3,)),
            *spread_sems,
            *spread_sems,
            dma((2,)),
            dma((4,)),
            dma((4,)),
            dma((1,)),
            dma((4, 4)),
            dma((1,)),
            dma((1,)),
            dma((1,)),
            dma((1,)),
            dma((1,)),
            dma((1,)),
        ],
        compiler_params=pltpu.CompilerParams(
            collective_id=0, has_side_effects=True, vmem_limit_bytes=60 * 1024 * 1024
        ),
        name="predict",
    )(
        token_ids,
        remask,
        mask_embed,
        gain_in.reshape(1, -1),
        gain_out.reshape(1, -1),
        table,
        w_qkv,
        w_out,
        position_embed,
    )
    log_probs, confidence, stats = pl.pallas_call(
        write_out,
        out_shape=(
            jax.ShapeDtypeStruct((1, 256, 256), BF),
            jax.ShapeDtypeStruct((1, 256), F32),
            jax.ShapeDtypeStruct((1, 2), F32),
        ),
        in_specs=[vmem] * 3,
        out_specs=(vmem, vmem, vmem),
        name="write_out",
    )(log_probs, confidence, stats)
    return log_probs, confidence, stats.reshape(2)


def solution(mesh):
    finer = Mesh(mesh.devices.reshape(8, 4, 4, 2, 2), AXES)
    frames = ("clip", "zl", "x")
    tm = ("zl", "x")
    mp = ("zh", "core")
    in_specs = (
        P(frames, None),
        P(frames, None),
        P(tm, None, None),
        P(),
        P(mp, None),
        P(),
        P(),
        P(None, None, mp),
        P(mp, None),
    )
    out_specs = (P(frames, None, mp), P(frames, None), P("clip"))
    return jax.shard_map(body, mesh=finer, in_specs=in_specs, out_specs=out_specs, check_vma=False)
```

```python
import math

import jax
import jax.numpy as jnp
from jax import lax
from jax.experimental import pallas as pl
from jax.experimental.pallas import tpu as pltpu
from jax.sharding import Mesh
from jax.sharding import PartitionSpec as P

HEAD_DIM = 64
MESH = pl.DeviceIdType.MESH
AXES = ("clip", "zl", "x", "zh", "core")
BF = jnp.bfloat16
F32 = jnp.float32
SCALE = HEAD_DIM**-0.5 * math.log2(math.e)


def coords():
    return [lax.axis_index(name) for name in AXES]


def at(y, zl, x, zh, core):
    mine = coords()
    sizes = (8, 4, 4, 2, 2)
    return tuple(
        lax.rem(mine[k] + step + sizes[k], sizes[k]) if step else mine[k]
        for k, step in enumerate((y, zl, x, zh, core))
    )


def mirror():
    y, zl, x, zh, core = coords()
    return (y, 3 - zl, x, 1 - zh, core)


def remote(src, dst, send, recv, device):
    return pltpu.make_async_remote_copy(
        src_ref=src, dst_ref=dst, send_sem=send, recv_sem=recv, device_id=device, device_id_type=MESH
    )


def arrived(ref, sem):
    remote(ref, ref, sem, sem, at(0, 0, 0, 0, 1)).wait_recv()


def left(ref, sem):
    remote(ref, ref, sem, sem, at(0, 0, 0, 0, 1)).wait_send()


def norm_rows(h, gain):
    center = h - jnp.mean(h, axis=-1, keepdims=True)
    spread = jnp.mean(center * center, axis=-1, keepdims=True)
    return center * lax.rsqrt(spread + 1e-05) * gain


class Spread:
    def __init__(self, hbm, full, first, ssem, zsem, y1sem, x1sem, y2sem, x2sem, dsem):
        self.hbm, self.full, self.first, self.ssem, self.zsem, self.dsem = hbm, full, first, ssem, zsem, dsem
        self.y1, self.x1, self.y2, self.x2 = y1sem, x1sem, y2sem, x2sem
        y, zl, x, zh, core = coords()
        self.yq, self.x = lax.rem(y, 4), x
        self.own = zh * 2 + core
        self.got = (1 - zh) * 2 + core

    def quarter(self, k):
        return pl.ds(pl.multiple_of(k * 256, 256), 256)

    def rows(self, quarter, x):
        return pl.ds(pl.multiple_of(quarter * 256 + x * 64, 64), 64)

    def cols(self, yq, half):
        return pl.ds(pl.multiple_of(half * 512 + yq * 128, 128), 128)

    def piece(self, x, yq, half):
        return self.full.at[self.rows(self.got, x), self.cols(yq, half)]

    def strip(self, yq, half):
        return self.full.at[self.quarter(self.got), self.cols(yq, half)]

    def block(self, x):
        return self.full.at[self.rows(self.got, x), pl.ds(0, 512)]

    def y_of(self, dy):
        return lax.rem(self.yq - dy + 8, 4)

    def x_of(self, dx):
        return lax.rem(self.x - dx + 4, 4)

    def local(self):
        return pltpu.make_async_copy(self.hbm, self.full.at[self.quarter(self.own)], self.ssem.at[4])

    def fetch(self, half):
        rows = pl.ds(pl.multiple_of(self.x * 64, 64), 64)
        return pltpu.make_async_copy(
            self.hbm.at[rows, self.cols(self.yq, half)], self.first.at[half], self.ssem.at[5 + half]
        )

    def start_z(self):
        for half in range(2):
            piece = self.full.at[self.rows(self.own, self.x), self.cols(self.yq, half)]
            remote(self.first.at[half], piece, self.ssem.at[0], self.zsem.at[half], mirror()).start()

    def start_own_quarter(self):
        self.hand_over(self.full.at[self.quarter(self.own)], 0)

    def hand_over(self, ref, k):
        remote(ref, ref, self.ssem.at[3], self.dsem.at[k], at(0, 0, 0, 0, 1)).start()

    def along_y(self, ref, sem, recv):
        for dy in (2, 1, 7):
            remote(ref, ref, self.ssem.at[sem], recv.at[dy], at(dy, 0, 0, 0, 0)).start()

    def along_x(self, ref, sem, recv):
        for dx in (2, 1, 3):
            remote(ref, ref, self.ssem.at[sem], recv.at[dx], at(0, 0, dx, 0, 0)).start()

    def begin(self):
        first, second = self.piece(self.x, self.yq, 0), self.piece(self.x, self.yq, 1)
        arrived(first, self.zsem.at[0])
        self.along_y(first, 1, self.y1)
        arrived(second, self.zsem.at[1])
        self.along_x(second, 1, self.x1)
        self.along_x(first, 2, self.x2)
        self.along_y(second, 2, self.y2)

    def forward(self):
        for dy, dx in ((1, 1), (7, 3), (2, 2)):
            first = self.piece(self.x, self.y_of(dy), 0)
            arrived(first, self.y1.at[dy])
            self.along_x(first, 2, self.x2)
            second = self.piece(self.x_of(dx), self.yq, 1)
            arrived(second, self.x1.at[dx])
            self.along_y(second, 2, self.y2)
        self.hand_over(self.block(self.x), 1)
        self.hand_over(self.strip(self.yq, 1), 1)

    def finish(self):
        for dy, dx in ((1, 1), (7, 3), (2, 2)):
            block = self.block(self.x_of(dx))
            arrived(block, self.x2.at[dx])
            self.hand_over(block, 1)
            strip = self.strip(self.y_of(dy), 1)
            arrived(strip, self.y2.at[dy])
            self.hand_over(strip, 1)

    def wait_sent(self):
        left(self.full.at[pl.ds(0, 64), pl.ds(0, 256)], self.ssem.at[0])
        left(self.full.at[pl.ds(0, 64), pl.ds(0, 768)], self.ssem.at[1])
        left(self.full.at[pl.ds(0, 192)], self.ssem.at[2])
        left(self.full.at[pl.ds(0, 512)], self.ssem.at[3])

    def begin_slow(self):
        for half in range(2):
            piece = self.piece(self.x, self.yq, half)
            arrived(piece, self.zsem.at[half])
            self.along_x(piece, 1, self.x1)

    def forward_slow(self):
        for dx in (1, 3, 2):
            arrived(self.full.at[self.rows(self.got, self.x_of(dx)), pl.ds(0, 256)], self.x1.at[dx])
        for half in range(2):
            self.along_y(self.strip(self.yq, half), 2, self.y2)

    def finish_slow(self):
        for dy in (1, 7, 2):
            arrived(self.full.at[self.quarter(self.got), pl.ds(0, 256)], self.y2.at[dy])
        self.hand_over(self.full.at[self.quarter(self.got)], 1)

    def wait_sent_slow(self):
        left(self.full.at[pl.ds(0, 64), pl.ds(0, 256)], self.ssem.at[0])
        left(self.full.at[pl.ds(0, 64), pl.ds(0, 768)], self.ssem.at[1])
        left(self.full.at[pl.ds(0, 256), pl.ds(0, 768)], self.ssem.at[2])
        left(self.full.at[pl.ds(0, 512)], self.ssem.at[3])

    def wait_all(self):
        quarter = self.full.at[pl.ds(0, 256)]
        arrived(quarter, self.dsem.at[0])
        arrived(quarter, self.dsem.at[1])


def kernel(
    ids_hbm, remask_hbm, mask_hbm, gain_in_hbm, gain_out_hbm, table_hbm, wqkv_hbm, wout_hbm, pos_hbm,
    logp_hbm, conf_hbm, stats_hbm,
    ids_ref, remask_ref, mask_embed_ref, gain_in_ref, gain_out_ref, logp_ref, conf_ref, stats_ref,
    table_first, wout_first, flipped, table, wout, wqkv, pos, hidden, normed, kv_out, q_out, kv, q_in, qpad, high, total, summed, o_out, ctx,
    final, logits, weight, stat_out, stat_in,
    local_sem, small_sem, put_sem,
    t_s, t_z, t_y1, t_x1, t_y2, t_x2, t_d, w_s, w_z, w_y1, w_x1, w_y2, w_x2, w_d,
    a_send, a_recv, q_recv, b_send, b_recv,
    c_send, c_recv, f_send, f_recv, s_send, s_recv,
):
    y, zl, x, zh, core = coords()
    mp = zh * 2 + core
    frame = zl * 4 + x
    pair_z = (zl, zl + 1 - 2 * lax.rem(zl, 2), lax.rem(zl + 2, 4), 3 - zl)
    tab = Spread(table_hbm, table, table_first, t_s, t_z, t_y1, t_x1, t_y2, t_x2, t_d)
    out = Spread(wout_hbm, wout, wout_first, w_s, w_z, w_y1, w_x1, w_y2, w_x2, w_d)
    load_pos = pltpu.make_async_copy(pos_hbm.at[0], pos, local_sem.at[0])
    load_qkv = pltpu.make_async_copy(wqkv_hbm, wqkv, local_sem.at[1])

    small = [
        pltpu.make_async_copy(src, dst, small_sem.at[k])
        for k, (src, dst) in enumerate(
            (
                (ids_hbm, ids_ref),
                (remask_hbm, remask_ref),
                (mask_hbm, mask_embed_ref),
                (gain_in_hbm, gain_in_ref),
                (gain_out_hbm, gain_out_ref),
            )
        )
    ]
    for half in range(2):
        tab.fetch(half).start()
    barrier = pltpu.get_barrier_semaphore()
    peers = []
    for k in range(1, 16):
        place = lax.rem(zh * 8 + zl * 2 + core + k, 16)
        peers.append((y, lax.rem(place // 2, 4), x, place // 8, lax.rem(place, 2)))
    peers += [at(k, 0, 0, 0, 0) for k in (1, 2, 6, 7)]
    peers += [at(0, dz, dx, 0, dc) for dx in range(1, 4) for dz in range(4) for dc in range(2)]
    for peer in peers:
        pl.semaphore_signal(barrier, inc=1, device_id=peer, device_id_type=MESH)
    tab.local().start()
    for copy in small:
        copy.start()
    load_pos.start()
    out.local().start()
    for half in range(2):
        out.fetch(half).start()
    load_qkv.start()
    for half in range(2):
        tab.fetch(half).wait()
    pl.semaphore_wait(barrier, len(peers))
    tab.start_z()
    tab.local().wait()
    tab.start_own_quarter()
    for copy in small:
        copy.wait()
    row = lax.broadcasted_iota(jnp.int32, (256, 256), 0)
    lane = lax.broadcasted_iota(jnp.int32, (256, 256), 1)
    masked = jnp.max(jnp.where(remask_ref[...] == row, 1.0, 0.0), axis=1, keepdims=True)
    ids_col = jnp.sum(
        jnp.where(row == lane, ids_ref[...].astype(F32), 0.0), axis=1, keepdims=True
    )
    weight[...] = jnp.broadcast_to(masked, (256, 128))
    ids_col = jnp.where(masked > 0.5, -1.0, ids_col)
    mask_row = mask_embed_ref[...].astype(F32).reshape(1, 1024)

    def looked_up(first, count):
        entry = lax.broadcasted_iota(jnp.int32, (256, count), 1) + first
        onehot = jnp.where(entry.astype(F32) == ids_col, 1.0, 0.0).astype(BF)
        rows = table[pl.ds(pl.multiple_of(first, count), count)]
        return jnp.dot(onehot, rows, preferred_element_type=F32)

    load_pos.wait()
    for k in range(4):
        block = slice(k * 64, k * 64 + 64)
        hidden[block] = pos[block].astype(F32) + jnp.where(masked[block] > 0.5, mask_row, 0.0)
    tab.begin()
    for half in range(2):
        out.fetch(half).wait()
    out.start_z()
    arrived(table.at[pl.ds(0, 256)], tab.dsem.at[0])
    hidden[...] += looked_up(zh * 512, 512)
    tab.forward()
    out.begin_slow()
    tab.finish()
    out.forward_slow()
    out.local().wait()
    out.start_own_quarter()
    load_qkv.wait()
    hidden[...] += looked_up((2 - 2 * zh + core) * 256, 256)
    arrived(table.at[pl.ds(0, 256)], tab.dsem.at[1])
    hidden[...] += looked_up((3 - 2 * zh - core) * 256, 256)
    gain_in = gain_in_ref[...]
    for k in range(4):
        block = slice(k * 64, k * 64 + 64)
        normed[block] = norm_rows(hidden[block], gain_in).astype(BF)
    low = lax.broadcasted_iota(jnp.int32, (256, 128), 1) < 64
    n_all = normed[...]
    keys = jnp.dot(n_all, wqkv[1], preferred_element_type=F32)
    values = jnp.dot(n_all, wqkv[2], preferred_element_type=F32)
    for g in range(2):
        kg, vg = keys[:, g * 128 : g * 128 + 128], values[:, g * 128 : g * 128 + 128]
        kv_out[2 * g] = jnp.where(low, kg, pltpu.roll(vg, 64, 1)).astype(BF)
        kv_out[2 * g + 1] = jnp.where(low, pltpu.roll(kg, 64, 1), vg).astype(BF)
    query = jnp.dot(n_all, wqkv[0], preferred_element_type=F32)
    low_half = low[:128]
    for g in range(2):
        qa, qb = query[:128, g * 128 : g * 128 + 128], query[128:, g * 128 : g * 128 + 128]
        q_out[2 * g] = jnp.where(low_half, qa, pltpu.roll(qb, 64, 1)).astype(BF)
        q_out[2 * g + 1] = jnp.where(low_half, pltpu.roll(qa, 64, 1), qb).astype(BF)
    def spot(s, slot):
        return (0, 2, 1, 3)[s] * 4 + slot

    chunk = {0: slice(0, 4), 2: slice(4, 8), 1: slice(8, 13), 3: slice(13, 16)}

    def pass_on(block, s):
        for dx in (1, 3, 2):
            slot = (0, 1, 3, 2)[dx]
            remote(block, kv.at[spot(s, slot)], b_send.at[0], b_recv.at[s, slot], at(0, 0, dx, 0, 0)).start()

    pass_on(kv_out.at[zl], 0)
    def send_keys(d):
        remote(
            kv_out.at[pair_z[d]], kv.at[spot(d, 0)], a_send.at[0], a_recv.at[d], (y, pair_z[d], x, zh, core)
        ).start()

    def send_query(d):
        remote(
            q_out.at[pair_z[d]], q_in.at[d], a_send.at[1], q_recv.at[d], (y, pair_z[d], x, zh, core)
        ).start()

    send_keys(2)
    send_keys(1)
    send_query(1)
    send_query(2)
    send_keys(3)
    send_query(3)
    kv[spot(0, 0)] = kv_out[zl]

    def unpack(k, packed):
        packed = packed.astype(F32)
        qpad[k, :128] = jnp.where(low_half, packed, 0.0).astype(BF)
        qpad[k, 128:] = jnp.where(low_half, pltpu.roll(packed, 64, 1), 0.0).astype(BF)

    unpack(0, q_out[zl])
    low64 = low[:64]
    head_here = mp * 4 + zl

    def take(s):
        arrived(kv.at[spot(s, 0)], a_recv.at[s])
        pass_on(kv.at[spot(s, 0)], s)

    held = set()

    def ready(s, b):
        if b and (b, "q") not in held:
            arrived(q_in.at[b], q_recv.at[b])
            unpack(b, q_in[b])
            held.add((b, "q"))
        if s not in held:
            for slot in (1, 2, 3):
                arrived(kv.at[spot(s, slot)], b_recv.at[s, slot])
            held.add(s)

    def score(s, b):
        return lax.dot_general(
            qpad[b], kv[chunk[s]].reshape(-1, 128), (((1,), (1,)), ((), ())), preferred_element_type=F32
        )

    def absorb(s, b, scores):
        rows = kv[chunk[s]].reshape(-1, 128)
        top = jnp.max(scores, axis=1, keepdims=True)
        if s == 0:
            w = jnp.exp2(scores * SCALE - top * SCALE)
            high[b] = jnp.broadcast_to(top, (256, 128))
            total[b] = jnp.broadcast_to(jnp.sum(w, axis=1, keepdims=True), (256, 128))
            summed[b] = jnp.dot(w.astype(BF), rows, preferred_element_type=F32)
            return
        before = high[b]
        now = jnp.maximum(before, top)
        fade = jnp.exp2((before - now) * SCALE)
        w = jnp.exp2(scores * SCALE - now[:, :1] * SCALE)
        sums = total[b] * fade + jnp.sum(w, axis=1, keepdims=True)
        acc = summed[b] * fade + jnp.dot(w.astype(BF), rows, preferred_element_type=F32)
        if s != 3:
            high[b], total[b], summed[b] = now, sums, acc
            return
        rows = acc / sums
        for half in range(2):
            top_rows = rows[half * 128 : half * 128 + 64]
            low_rows = rows[half * 128 + 64 : half * 128 + 128]
            o_out[b, half] = jnp.where(low64, pltpu.roll(top_rows, 64, 1), low_rows).astype(BF)

    def send_context(b):
        for dh in (1, 0):
            for dc in (0, 1):
                if b == 0 and dh == 0 and dc == 0:
                    continue
                half = lax.rem(core + dc, 2)
                there = (y, pair_z[b], x, lax.rem(zh + dh, 2), half)
                remote(
                    o_out.at[b, half], ctx.at[head_here], c_send.at[0], c_recv.at[0], there
                ).start()

    steps = [(s, b) for s in (0, 2) for b in (0, 1, 2)] + [(0, 3), (2, 3)]
    steps += [(s, b) for s in (1, 3) for b in (2, 3, 1, 0)]
    take(2)
    take(1)
    ready(0, 0)
    scores = score(0, 0)
    for i, (s, b) in enumerate(steps):
        if i + 1 < len(steps):
            if steps[i + 1] == (2, 0):
                take(3)
            ready(*steps[i + 1])
            following = score(*steps[i + 1])
        absorb(s, b, scores)
        if s == 3:
            send_context(b)
        scores = following
    ctx[head_here] = o_out[0, core]
    out.finish_slow()
    for q in range(4):
        flipped[:, q * 256 : q * 256 + 256] = table[q * 256 : q * 256 + 256].T
    out.wait_all()

    arrived(ctx.at[pl.ds(0, 15)], c_recv.at[0])
    pieces = []
    for g in range(8):
        a, b = ctx[2 * g].astype(F32), ctx[2 * g + 1].astype(F32)
        pieces.append(
            jnp.concatenate(
                [
                    jnp.where(low64, a, pltpu.roll(b, 64, 1)),
                    jnp.where(low64, pltpu.roll(a, 64, 1), b),
                ],
                axis=0,
            ).astype(BF)
        )
    context = jnp.concatenate(pieces, axis=1)
    mine = pl.ds(pl.multiple_of(core * 128, 128), 128)
    h = hidden[mine] + jnp.dot(context, wout[...], preferred_element_type=F32)
    final[mine] = norm_rows(h, gain_out_ref[...]).astype(BF)
    send_final = remote(final.at[mine], final.at[mine], f_send.at[0], f_recv.at[0], at(0, 0, 0, 0, 1))
    send_final.start()

    def finish(block):
        rows = final[block]
        tops = []
        for q in range(4):
            part = jnp.dot(rows, flipped[:, q * 256 : q * 256 + 256], preferred_element_type=F32)
            logits[q, block] = part
            tops.append(jnp.max(part, axis=1, keepdims=True))
        top = jnp.maximum(jnp.maximum(tops[0], tops[1]), jnp.maximum(tops[2], tops[3]))
        sums = jnp.zeros_like(top)
        for q in range(4):
            sums = sums + jnp.sum(jnp.exp(logits[q, block] - top), axis=1, keepdims=True)
        lse = top + jnp.log(sums)
        conf = jnp.exp(top - lse)
        high[0, block] = jnp.broadcast_to(conf, (128, 128))
        return conf, lse

    def put_rows(block, lse):
        logp_ref[block] = (logits[mp, block] - lse).astype(BF)

    conf, lse = finish(mine)
    w = weight[mine][:, :1]
    lane1 = lax.broadcasted_iota(jnp.int32, (1, 128), 1)
    conf_sum = jnp.sum(conf * w, axis=0, keepdims=True)
    count = jnp.sum(w, axis=0, keepdims=True)
    tile = jnp.where(lane1 == 0, conf_sum, jnp.where(lane1 == 1, count, 0.0))
    place = frame * 2 + core
    stat_out[...] = tile
    stat_in[place] = tile
    for dz in (2, 3, 1, 0):
        for dx in (2, 3, 1, 0):
            for dc in range(2):
                if dz or dx or dc:
                    remote(
                        stat_out, stat_in.at[place], s_send.at[0], s_recv.at[0], at(0, dz, dx, 0, dc)
                    ).start()
    put_rows(mine, lse)
    other = pl.ds(pl.multiple_of((1 - core) * 128, 128), 128)
    arrived(final.at[other], f_recv.at[0])
    conf, lse = finish(other)
    put_rows(other, lse)
    conf_ref[...] = jnp.sum(jnp.where(row == lane, high[0][:, :1], 0.0), axis=0, keepdims=True)
    put = [
        pltpu.make_async_copy(logp_ref, logp_hbm.at[0], put_sem.at[0]),
        pltpu.make_async_copy(conf_ref, conf_hbm, put_sem.at[1]),
        pltpu.make_async_copy(stats_ref, stats_hbm, put_sem.at[2]),
    ]
    put[0].start()
    put[1].start()
    tab.wait_sent()
    out.wait_sent_slow()
    left(kv_out.at[pl.ds(0, 3)], a_send.at[0])
    left(q_out.at[pl.ds(0, 3)], a_send.at[1])
    left(kv.at[pl.ds(0, 12)], b_send.at[0])
    left(ctx.at[pl.ds(0, 15)], c_send.at[0])
    send_final.wait_send()
    arrived(stat_in.at[pl.ds(0, 31)], s_recv.at[0])
    left(stat_in.at[pl.ds(0, 31)], s_send.at[0])
    sums = stat_in[0]
    for k in range(1, 32):
        sums = sums + stat_in[k]
    all_conf = jnp.sum(jnp.where(lane1 == 0, sums, 0.0), axis=1, keepdims=True)
    all_count = jnp.sum(jnp.where(lane1 == 1, sums, 0.0), axis=1, keepdims=True)
    stats_ref[...] = jnp.where(lane1 == 0, all_conf / all_count, jnp.log(all_count / 4096.0))
    put[2].start()
    for copy in put:
        copy.wait()


def write_out(logp, conf, stats, logp_out, conf_out, stats_out):
    logp_out[...] = logp[...]
    conf_out[...] = conf[...]
    stats_out[...] = stats[:, :2]


def body(token_ids, remask, position_embed, mask_embed, table, gain_in, gain_out, w_qkv, w_out):
    vmem = pl.BlockSpec(memory_space=pltpu.VMEM)
    hbm = pl.BlockSpec(memory_space=pl.ANY)
    dma = pltpu.SemaphoreType.DMA
    spread_sems = [dma((7,)), dma((2,)), dma((8,)), dma((4,)), dma((8,)), dma((4,)), dma((2,))]
    log_probs, confidence, stats = pl.pallas_call(
        kernel,
        out_shape=(
            jax.ShapeDtypeStruct((1, 256, 256), BF),
            jax.ShapeDtypeStruct((1, 256), F32),
            jax.ShapeDtypeStruct((1, 128), F32),
        ),
        in_specs=[hbm] * 9,
        out_specs=(hbm, hbm, hbm),
        scratch_shapes=[
            pltpu.VMEM((1, 256), jnp.int32),
            pltpu.VMEM((1, 256), jnp.int32),
            pltpu.VMEM((1024,), BF),
            pltpu.VMEM((1, 1024), F32),
            pltpu.VMEM((1, 1024), F32),
            pltpu.VMEM((256, 256), BF),
            pltpu.VMEM((1, 256), F32),
            pltpu.VMEM((1, 128), F32),
            pltpu.VMEM((2, 64, 128), BF),
            pltpu.VMEM((2, 64, 128), BF),
            pltpu.VMEM((1024, 1024), BF),
            pltpu.VMEM((1024, 1024), BF),
            pltpu.VMEM((1024, 1024), BF),
            pltpu.VMEM((3, 1024, 256), BF),
            pltpu.VMEM((256, 1024), BF),
            pltpu.VMEM((256, 1024), F32),
            pltpu.VMEM((256, 1024), BF),
            pltpu.VMEM((4, 256, 128), BF),
            pltpu.VMEM((4, 128, 128), BF),
            pltpu.VMEM((16, 256, 128), BF),
            pltpu.VMEM((4, 128, 128), BF),
            pltpu.VMEM((4, 256, 128), BF),
            pltpu.VMEM((4, 256, 128), F32),
            pltpu.VMEM((4, 256, 128), F32),
            pltpu.VMEM((4, 256, 128), F32),
            pltpu.VMEM((4, 2, 64, 128), BF),
            pltpu.VMEM((16, 64, 128), BF),
            pltpu.VMEM((256, 1024), BF),
            pltpu.VMEM((4, 256, 256), F32),
            pltpu.VMEM((256, 128), F32),
            pltpu.VMEM((1, 128), F32),
            pltpu.VMEM((32, 1, 128), F32),
            dma((2,)),
            dma((5,)),
            dma((3,)),
            *spread_sems,
            *spread_sems,
            dma((2,)),
            dma((4,)),
            dma((4,)),
            dma((1,)),
            dma((4, 4)),
            dma((1,)),
            dma((1,)),
            dma((1,)),
            dma((1,)),
            dma((1,)),
            dma((1,)),
        ],
        compiler_params=pltpu.CompilerParams(
            collective_id=0, has_side_effects=True, vmem_limit_bytes=60 * 1024 * 1024
        ),
        name="predict",
    )(
        token_ids,
        remask,
        mask_embed,
        gain_in.reshape(1, -1),
        gain_out.reshape(1, -1),
        table,
        w_qkv,
        w_out,
        position_embed,
    )
    log_probs, confidence, stats = pl.pallas_call(
        write_out,
        out_shape=(
            jax.ShapeDtypeStruct((1, 256, 256), BF),
            jax.ShapeDtypeStruct((1, 256), F32),
            jax.ShapeDtypeStruct((1, 2), F32),
        ),
        in_specs=[vmem] * 3,
        out_specs=(vmem, vmem, vmem),
        name="write_out",
    )(log_probs, confidence, stats)
    return log_probs, confidence, stats.reshape(2)


def solution(mesh):
    finer = Mesh(mesh.devices.reshape(8, 4, 4, 2, 2), AXES)
    frames = ("clip", "zl", "x")
    tm = ("zl", "x")
    mp = ("zh", "core")
    in_specs = (
        P(frames, None),
        P(frames, None),
        P(tm, None, None),
        P(),
        P(mp, None),
        P(),
        P(),
        P(None, None, mp),
        P(mp, None),
    )
    out_specs = (P(frames, None, mp), P(frames, None), P("clip"))
    return jax.shard_map(body, mesh=finer, in_specs=in_specs, out_specs=out_specs, check_vma=False)
```

```python
import math

import jax
import jax.numpy as jnp
from jax import lax
from jax.experimental import pallas as pl
from jax.experimental.pallas import tpu as pltpu
from jax.sharding import Mesh
from jax.sharding import PartitionSpec as P

HEAD_DIM = 64
MESH = pl.DeviceIdType.MESH
AXES = ("clip", "zl", "x", "zh", "core")
BF = jnp.bfloat16
F32 = jnp.float32
SCALE = HEAD_DIM**-0.5 * math.log2(math.e)


def coords():
    return [lax.axis_index(name) for name in AXES]


def at(y, zl, x, zh, core):
    mine = coords()
    sizes = (8, 4, 4, 2, 2)
    return tuple(
        lax.rem(mine[k] + step + sizes[k], sizes[k]) if step else mine[k]
        for k, step in enumerate((y, zl, x, zh, core))
    )


def mirror():
    y, zl, x, zh, core = coords()
    return (y, 3 - zl, x, 1 - zh, core)


def remote(src, dst, send, recv, device):
    return pltpu.make_async_remote_copy(
        src_ref=src, dst_ref=dst, send_sem=send, recv_sem=recv, device_id=device, device_id_type=MESH
    )


def arrived(ref, sem):
    remote(ref, ref, sem, sem, at(0, 0, 0, 0, 1)).wait_recv()


def left(ref, sem):
    remote(ref, ref, sem, sem, at(0, 0, 0, 0, 1)).wait_send()


def norm_rows(h, gain):
    center = h - jnp.mean(h, axis=-1, keepdims=True)
    spread = jnp.mean(center * center, axis=-1, keepdims=True)
    return center * lax.rsqrt(spread + 1e-05) * gain


class Spread:
    def __init__(self, hbm, full, first, ssem, zsem, y1sem, x1sem, y2sem, x2sem, dsem):
        self.hbm, self.full, self.first, self.ssem, self.zsem, self.dsem = hbm, full, first, ssem, zsem, dsem
        self.y1, self.x1, self.y2, self.x2 = y1sem, x1sem, y2sem, x2sem
        y, zl, x, zh, core = coords()
        self.yq, self.x = lax.rem(y, 4), x
        self.own = zh * 2 + core
        self.got = (1 - zh) * 2 + core

    def quarter(self, k):
        return pl.ds(pl.multiple_of(k * 256, 256), 256)

    def rows(self, quarter, x):
        return pl.ds(pl.multiple_of(quarter * 256 + x * 64, 64), 64)

    def cols(self, yq, half):
        return pl.ds(pl.multiple_of(half * 512 + yq * 128, 128), 128)

    def piece(self, x, yq, half):
        return self.full.at[self.rows(self.got, x), self.cols(yq, half)]

    def strip(self, yq, half):
        return self.full.at[self.quarter(self.got), self.cols(yq, half)]

    def block(self, x):
        return self.full.at[self.rows(self.got, x), pl.ds(0, 512)]

    def y_of(self, dy):
        return lax.rem(self.yq - dy + 8, 4)

    def x_of(self, dx):
        return lax.rem(self.x - dx + 4, 4)

    def local(self):
        return pltpu.make_async_copy(self.hbm, self.full.at[self.quarter(self.own)], self.ssem.at[4])

    def fetch(self, half):
        rows = pl.ds(pl.multiple_of(self.x * 64, 64), 64)
        return pltpu.make_async_copy(
            self.hbm.at[rows, self.cols(self.yq, half)], self.first.at[half], self.ssem.at[5 + half]
        )

    def start_z(self):
        for half in range(2):
            piece = self.full.at[self.rows(self.own, self.x), self.cols(self.yq, half)]
            remote(self.first.at[half], piece, self.ssem.at[0], self.zsem.at[half], mirror()).start()

    def start_own_quarter(self):
        self.hand_over(self.full.at[self.quarter(self.own)], 0)

    def hand_over(self, ref, k):
        remote(ref, ref, self.ssem.at[3], self.dsem.at[k], at(0, 0, 0, 0, 1)).start()

    def along_y(self, ref, sem, recv):
        for dy in (2, 1, 7):
            remote(ref, ref, self.ssem.at[sem], recv.at[dy], at(dy, 0, 0, 0, 0)).start()

    def along_x(self, ref, sem, recv):
        for dx in (2, 1, 3):
            remote(ref, ref, self.ssem.at[sem], recv.at[dx], at(0, 0, dx, 0, 0)).start()

    def begin(self):
        first, second = self.piece(self.x, self.yq, 0), self.piece(self.x, self.yq, 1)
        arrived(first, self.zsem.at[0])
        self.along_y(first, 1, self.y1)
        arrived(second, self.zsem.at[1])
        self.along_x(second, 1, self.x1)
        self.along_x(first, 2, self.x2)
        self.along_y(second, 2, self.y2)

    def forward(self):
        for dy, dx in ((1, 1), (7, 3), (2, 2)):
            first = self.piece(self.x, self.y_of(dy), 0)
            arrived(first, self.y1.at[dy])
            self.along_x(first, 2, self.x2)
            second = self.piece(self.x_of(dx), self.yq, 1)
            arrived(second, self.x1.at[dx])
            self.along_y(second, 2, self.y2)
        self.hand_over(self.block(self.x), 1)
        self.hand_over(self.strip(self.yq, 1), 1)

    def finish(self):
        for dy, dx in ((1, 1), (7, 3), (2, 2)):
            block = self.block(self.x_of(dx))
            arrived(block, self.x2.at[dx])
            self.hand_over(block, 1)
            strip = self.strip(self.y_of(dy), 1)
            arrived(strip, self.y2.at[dy])
            self.hand_over(strip, 1)

    def wait_sent(self):
        left(self.full.at[pl.ds(0, 64), pl.ds(0, 256)], self.ssem.at[0])
        left(self.full.at[pl.ds(0, 64), pl.ds(0, 768)], self.ssem.at[1])
        left(self.full.at[pl.ds(0, 192)], self.ssem.at[2])
        left(self.full.at[pl.ds(0, 512)], self.ssem.at[3])

    def begin_slow(self):
        for half in range(2):
            piece = self.piece(self.x, self.yq, half)
            arrived(piece, self.zsem.at[half])
            self.along_x(piece, 1, self.x1)

    def forward_slow(self):
        for dx in (1, 3, 2):
            arrived(self.full.at[self.rows(self.got, self.x_of(dx)), pl.ds(0, 256)], self.x1.at[dx])
        for half in range(2):
            self.along_y(self.strip(self.yq, half), 2, self.y2)

    def finish_slow(self):
        for dy in (1, 7, 2):
            arrived(self.full.at[self.quarter(self.got), pl.ds(0, 256)], self.y2.at[dy])
        self.hand_over(self.full.at[self.quarter(self.got)], 1)

    def wait_sent_slow(self):
        left(self.full.at[pl.ds(0, 64), pl.ds(0, 256)], self.ssem.at[0])
        left(self.full.at[pl.ds(0, 64), pl.ds(0, 768)], self.ssem.at[1])
        left(self.full.at[pl.ds(0, 256), pl.ds(0, 768)], self.ssem.at[2])
        left(self.full.at[pl.ds(0, 512)], self.ssem.at[3])

    def wait_all(self):
        quarter = self.full.at[pl.ds(0, 256)]
        arrived(quarter, self.dsem.at[0])
        arrived(quarter, self.dsem.at[1])


def kernel(
    ids_hbm, remask_hbm, mask_hbm, gain_in_hbm, gain_out_hbm, table_hbm, wqkv_hbm, wout_hbm, pos_hbm,
    logp_ref, conf_ref, stats_ref,
    ids_ref, remask_ref, mask_embed_ref, gain_in_ref, gain_out_ref,
    table_first, wout_first, flipped, table, wout, wqkv, pos, hidden, normed, kv_out, q_out, kv, q_in, qpad, high, total, summed, o_out, ctx,
    final, logits, weight, stat_out, stat_in,
    local_sem, small_sem,
    t_s, t_z, t_y1, t_x1, t_y2, t_x2, t_d, w_s, w_z, w_y1, w_x1, w_y2, w_x2, w_d,
    a_send, a_recv, q_recv, b_send, b_recv,
    c_send, c_recv, f_send, f_recv, s_send, s_recv,
):
    y, zl, x, zh, core = coords()
    mp = zh * 2 + core
    frame = zl * 4 + x
    pair_z = (zl, zl + 1 - 2 * lax.rem(zl, 2), lax.rem(zl + 2, 4), 3 - zl)
    tab = Spread(table_hbm, table, table_first, t_s, t_z, t_y1, t_x1, t_y2, t_x2, t_d)
    out = Spread(wout_hbm, wout, wout_first, w_s, w_z, w_y1, w_x1, w_y2, w_x2, w_d)
    load_pos = pltpu.make_async_copy(pos_hbm.at[0], pos, local_sem.at[0])
    load_qkv = pltpu.make_async_copy(wqkv_hbm, wqkv, local_sem.at[1])

    small = [
        pltpu.make_async_copy(src, dst, small_sem.at[k])
        for k, (src, dst) in enumerate(
            (
                (ids_hbm, ids_ref),
                (remask_hbm, remask_ref),
                (mask_hbm, mask_embed_ref),
                (gain_in_hbm, gain_in_ref),
                (gain_out_hbm, gain_out_ref),
            )
        )
    ]
    for half in range(2):
        tab.fetch(half).start()
    barrier = pltpu.get_barrier_semaphore()
    peers = []
    for k in range(1, 16):
        place = lax.rem(zh * 8 + zl * 2 + core + k, 16)
        peers.append((y, lax.rem(place // 2, 4), x, place // 8, lax.rem(place, 2)))
    peers += [at(k, 0, 0, 0, 0) for k in (1, 2, 6, 7)]
    peers += [at(0, dz, dx, 0, dc) for dx in range(1, 4) for dz in range(4) for dc in range(2)]
    for peer in peers:
        pl.semaphore_signal(barrier, inc=1, device_id=peer, device_id_type=MESH)
    tab.local().start()
    for copy in small:
        copy.start()
    load_pos.start()
    out.local().start()
    for half in range(2):
        out.fetch(half).start()
    load_qkv.start()
    for half in range(2):
        tab.fetch(half).wait()
    pl.semaphore_wait(barrier, len(peers))
    tab.start_z()
    tab.local().wait()
    tab.start_own_quarter()
    for copy in small:
        copy.wait()
    row = lax.broadcasted_iota(jnp.int32, (256, 256), 0)
    lane = lax.broadcasted_iota(jnp.int32, (256, 256), 1)
    masked = jnp.max(jnp.where(remask_ref[...] == row, 1.0, 0.0), axis=1, keepdims=True)
    ids_col = jnp.sum(
        jnp.where(row == lane, ids_ref[...].astype(F32), 0.0), axis=1, keepdims=True
    )
    weight[...] = jnp.broadcast_to(masked, (256, 128))
    ids_col = jnp.where(masked > 0.5, -1.0, ids_col)
    mask_row = mask_embed_ref[...].astype(F32).reshape(1, 1024)

    def looked_up(first, count):
        entry = lax.broadcasted_iota(jnp.int32, (256, count), 1) + first
        onehot = jnp.where(entry.astype(F32) == ids_col, 1.0, 0.0).astype(BF)
        rows = table[pl.ds(pl.multiple_of(first, count), count)]
        return jnp.dot(onehot, rows, preferred_element_type=F32)

    load_pos.wait()
    for k in range(4):
        block = slice(k * 64, k * 64 + 64)
        hidden[block] = pos[block].astype(F32) + jnp.where(masked[block] > 0.5, mask_row, 0.0)
    tab.begin()
    for half in range(2):
        out.fetch(half).wait()
    out.start_z()
    arrived(table.at[pl.ds(0, 256)], tab.dsem.at[0])
    hidden[...] += looked_up(zh * 512, 512)
    tab.forward()
    out.begin_slow()
    tab.finish()
    out.forward_slow()
    out.local().wait()
    out.start_own_quarter()
    load_qkv.wait()
    hidden[...] += looked_up((2 - 2 * zh + core) * 256, 256)
    arrived(table.at[pl.ds(0, 256)], tab.dsem.at[1])
    hidden[...] += looked_up((3 - 2 * zh - core) * 256, 256)
    gain_in = gain_in_ref[...]
    for k in range(4):
        block = slice(k * 64, k * 64 + 64)
        normed[block] = norm_rows(hidden[block], gain_in).astype(BF)
    low = lax.broadcasted_iota(jnp.int32, (256, 128), 1) < 64
    n_all = normed[...]
    keys = jnp.dot(n_all, wqkv[1], preferred_element_type=F32)
    values = jnp.dot(n_all, wqkv[2], preferred_element_type=F32)
    for g in range(2):
        kg, vg = keys[:, g * 128 : g * 128 + 128], values[:, g * 128 : g * 128 + 128]
        kv_out[2 * g] = jnp.where(low, kg, pltpu.roll(vg, 64, 1)).astype(BF)
        kv_out[2 * g + 1] = jnp.where(low, pltpu.roll(kg, 64, 1), vg).astype(BF)
    query = jnp.dot(n_all, wqkv[0], preferred_element_type=F32)
    low_half = low[:128]
    for g in range(2):
        qa, qb = query[:128, g * 128 : g * 128 + 128], query[128:, g * 128 : g * 128 + 128]
        q_out[2 * g] = jnp.where(low_half, qa, pltpu.roll(qb, 64, 1)).astype(BF)
        q_out[2 * g + 1] = jnp.where(low_half, pltpu.roll(qa, 64, 1), qb).astype(BF)
    def spot(s, slot):
        return (0, 2, 1, 3)[s] * 4 + slot

    chunk = {0: slice(0, 4), 2: slice(4, 8), 1: slice(8, 13), 3: slice(13, 16)}

    def pass_on(block, s):
        for dx in (1, 3, 2):
            slot = (0, 1, 3, 2)[dx]
            remote(block, kv.at[spot(s, slot)], b_send.at[0], b_recv.at[s, slot], at(0, 0, dx, 0, 0)).start()

    pass_on(kv_out.at[zl], 0)
    def send_keys(d):
        remote(
            kv_out.at[pair_z[d]], kv.at[spot(d, 0)], a_send.at[0], a_recv.at[d], (y, pair_z[d], x, zh, core)
        ).start()

    def send_query(d):
        remote(
            q_out.at[pair_z[d]], q_in.at[d], a_send.at[1], q_recv.at[d], (y, pair_z[d], x, zh, core)
        ).start()

    send_keys(2)
    send_keys(1)
    send_query(1)
    send_query(2)
    send_keys(3)
    send_query(3)
    kv[spot(0, 0)] = kv_out[zl]

    def unpack(k, packed):
        packed = packed.astype(F32)
        qpad[k, :128] = jnp.where(low_half, packed, 0.0).astype(BF)
        qpad[k, 128:] = jnp.where(low_half, pltpu.roll(packed, 64, 1), 0.0).astype(BF)

    unpack(0, q_out[zl])
    low64 = low[:64]
    head_here = mp * 4 + zl

    def take(s):
        arrived(kv.at[spot(s, 0)], a_recv.at[s])
        pass_on(kv.at[spot(s, 0)], s)

    held = set()

    def ready(s, b):
        if b and (b, "q") not in held:
            arrived(q_in.at[b], q_recv.at[b])
            unpack(b, q_in[b])
            held.add((b, "q"))
        if s not in held:
            for slot in (1, 2, 3):
                arrived(kv.at[spot(s, slot)], b_recv.at[s, slot])
            held.add(s)

    def score(s, b):
        return lax.dot_general(
            qpad[b], kv[chunk[s]].reshape(-1, 128), (((1,), (1,)), ((), ())), preferred_element_type=F32
        )

    def absorb(s, b, scores):
        rows = kv[chunk[s]].reshape(-1, 128)
        top = jnp.max(scores, axis=1, keepdims=True)
        if s == 0:
            w = jnp.exp2(scores * SCALE - top * SCALE)
            high[b] = jnp.broadcast_to(top, (256, 128))
            total[b] = jnp.broadcast_to(jnp.sum(w, axis=1, keepdims=True), (256, 128))
            summed[b] = jnp.dot(w.astype(BF), rows, preferred_element_type=F32)
            return
        before = high[b]
        now = jnp.maximum(before, top)
        fade = jnp.exp2((before - now) * SCALE)
        w = jnp.exp2(scores * SCALE - now[:, :1] * SCALE)
        sums = total[b] * fade + jnp.sum(w, axis=1, keepdims=True)
        acc = summed[b] * fade + jnp.dot(w.astype(BF), rows, preferred_element_type=F32)
        if s != 3:
            high[b], total[b], summed[b] = now, sums, acc
            return
        rows = acc / sums
        for half in range(2):
            top_rows = rows[half * 128 : half * 128 + 64]
            low_rows = rows[half * 128 + 64 : half * 128 + 128]
            o_out[b, half] = jnp.where(low64, pltpu.roll(top_rows, 64, 1), low_rows).astype(BF)

    def send_context(b):
        for dh in (1, 0):
            for dc in (0, 1):
                if b == 0 and dh == 0 and dc == 0:
                    continue
                half = lax.rem(core + dc, 2)
                there = (y, pair_z[b], x, lax.rem(zh + dh, 2), half)
                remote(
                    o_out.at[b, half], ctx.at[head_here], c_send.at[0], c_recv.at[0], there
                ).start()

    steps = [(s, b) for s in (0, 2) for b in (0, 1, 2)] + [(0, 3), (2, 3)]
    steps += [(s, b) for s in (1, 3) for b in (2, 3, 1, 0)]
    take(2)
    take(1)
    ready(0, 0)
    scores = score(0, 0)
    for i, (s, b) in enumerate(steps):
        if i + 1 < len(steps):
            if steps[i + 1] == (2, 0):
                take(3)
            ready(*steps[i + 1])
            following = score(*steps[i + 1])
        absorb(s, b, scores)
        if s == 3:
            send_context(b)
        scores = following
    ctx[head_here] = o_out[0, core]
    out.finish_slow()
    for q in range(4):
        flipped[:, q * 256 : q * 256 + 256] = table[q * 256 : q * 256 + 256].T
    out.wait_all()

    arrived(ctx.at[pl.ds(0, 15)], c_recv.at[0])
    pieces = []
    for g in range(8):
        a, b = ctx[2 * g].astype(F32), ctx[2 * g + 1].astype(F32)
        pieces.append(
            jnp.concatenate(
                [
                    jnp.where(low64, a, pltpu.roll(b, 64, 1)),
                    jnp.where(low64, pltpu.roll(a, 64, 1), b),
                ],
                axis=0,
            ).astype(BF)
        )
    context = jnp.concatenate(pieces, axis=1)
    mine = pl.ds(pl.multiple_of(core * 128, 128), 128)
    h = hidden[mine] + jnp.dot(context, wout[...], preferred_element_type=F32)
    final[mine] = norm_rows(h, gain_out_ref[...]).astype(BF)
    send_final = remote(final.at[mine], final.at[mine], f_send.at[0], f_recv.at[0], at(0, 0, 0, 0, 1))
    send_final.start()

    def finish(block):
        rows = final[block]
        tops = []
        for q in range(4):
            part = jnp.dot(rows, flipped[:, q * 256 : q * 256 + 256], preferred_element_type=F32)
            logits[q, block] = part
            tops.append(jnp.max(part, axis=1, keepdims=True))
        top = jnp.maximum(jnp.maximum(tops[0], tops[1]), jnp.maximum(tops[2], tops[3]))
        sums = jnp.zeros_like(top)
        for q in range(4):
            sums = sums + jnp.sum(jnp.exp(logits[q, block] - top), axis=1, keepdims=True)
        lse = top + jnp.log(sums)
        conf = jnp.exp(top - lse)
        high[0, block] = jnp.broadcast_to(conf, (128, 128))
        return conf, lse

    def put_rows(block, lse):
        logp_ref[block] = (logits[mp, block] - lse).astype(BF)

    conf, lse = finish(mine)
    w = weight[mine][:, :1]
    lane1 = lax.broadcasted_iota(jnp.int32, (1, 128), 1)
    conf_sum = jnp.sum(conf * w, axis=0, keepdims=True)
    count = jnp.sum(w, axis=0, keepdims=True)
    tile = jnp.where(lane1 == 0, conf_sum, jnp.where(lane1 == 1, count, 0.0))
    place = frame * 2 + core
    stat_out[...] = tile
    stat_in[place] = tile
    for dz in (2, 3, 1, 0):
        for dx in (2, 3, 1, 0):
            for dc in range(2):
                if dz or dx or dc:
                    remote(
                        stat_out, stat_in.at[place], s_send.at[0], s_recv.at[0], at(0, dz, dx, 0, dc)
                    ).start()
    put_rows(mine, lse)
    other = pl.ds(pl.multiple_of((1 - core) * 128, 128), 128)
    arrived(final.at[other], f_recv.at[0])
    conf, lse = finish(other)
    put_rows(other, lse)
    conf_ref[...] = jnp.sum(jnp.where(row == lane, high[0][:, :1], 0.0), axis=0, keepdims=True)
    tab.wait_sent()
    out.wait_sent_slow()
    left(kv_out.at[pl.ds(0, 3)], a_send.at[0])
    left(q_out.at[pl.ds(0, 3)], a_send.at[1])
    left(kv.at[pl.ds(0, 12)], b_send.at[0])
    left(ctx.at[pl.ds(0, 15)], c_send.at[0])
    send_final.wait_send()
    arrived(stat_in.at[pl.ds(0, 31)], s_recv.at[0])
    left(stat_in.at[pl.ds(0, 31)], s_send.at[0])
    sums = stat_in[0]
    for k in range(1, 32):
        sums = sums + stat_in[k]
    all_conf = jnp.sum(jnp.where(lane1 == 0, sums, 0.0), axis=1, keepdims=True)
    all_count = jnp.sum(jnp.where(lane1 == 1, sums, 0.0), axis=1, keepdims=True)
    both = jnp.where(lane1 == 0, all_conf / all_count, jnp.log(all_count / 4096.0))
    stats_ref[...] = both[:, :2]


def write_out(logp, conf, stats, logp_out, conf_out, stats_out, sem):
    copies = [
        pltpu.make_async_copy(src, dst, sem.at[k])
        for k, (src, dst) in enumerate(((logp, logp_out.at[0]), (conf, conf_out), (stats, stats_out)))
    ]
    for copy in copies:
        copy.start()
    for copy in copies:
        copy.wait()


def body(token_ids, remask, position_embed, mask_embed, table, gain_in, gain_out, w_qkv, w_out):
    vmem = pl.BlockSpec(memory_space=pltpu.VMEM)
    hbm = pl.BlockSpec(memory_space=pl.ANY)
    dma = pltpu.SemaphoreType.DMA
    spread_sems = [dma((7,)), dma((2,)), dma((8,)), dma((4,)), dma((8,)), dma((4,)), dma((2,))]
    log_probs, confidence, stats = pl.pallas_call(
        kernel,
        out_shape=(
            pltpu.VMEM((256, 256), BF),
            pltpu.VMEM((1, 256), F32),
            pltpu.VMEM((1, 2), F32),
        ),
        in_specs=[hbm] * 9,
        out_specs=(vmem, vmem, vmem),
        scratch_shapes=[
            pltpu.VMEM((1, 256), jnp.int32),
            pltpu.VMEM((1, 256), jnp.int32),
            pltpu.VMEM((1024,), BF),
            pltpu.VMEM((1, 1024), F32),
            pltpu.VMEM((1, 1024), F32),
            pltpu.VMEM((2, 64, 128), BF),
            pltpu.VMEM((2, 64, 128), BF),
            pltpu.VMEM((1024, 1024), BF),
            pltpu.VMEM((1024, 1024), BF),
            pltpu.VMEM((1024, 1024), BF),
            pltpu.VMEM((3, 1024, 256), BF),
            pltpu.VMEM((256, 1024), BF),
            pltpu.VMEM((256, 1024), F32),
            pltpu.VMEM((256, 1024), BF),
            pltpu.VMEM((4, 256, 128), BF),
            pltpu.VMEM((4, 128, 128), BF),
            pltpu.VMEM((16, 256, 128), BF),
            pltpu.VMEM((4, 128, 128), BF),
            pltpu.VMEM((4, 256, 128), BF),
            pltpu.VMEM((4, 256, 128), F32),
            pltpu.VMEM((4, 256, 128), F32),
            pltpu.VMEM((4, 256, 128), F32),
            pltpu.VMEM((4, 2, 64, 128), BF),
            pltpu.VMEM((16, 64, 128), BF),
            pltpu.VMEM((256, 1024), BF),
            pltpu.VMEM((4, 256, 256), F32),
            pltpu.VMEM((256, 128), F32),
            pltpu.VMEM((1, 128), F32),
            pltpu.VMEM((32, 1, 128), F32),
            dma((2,)),
            dma((5,)),
            *spread_sems,
            *spread_sems,
            dma((2,)),
            dma((4,)),
            dma((4,)),
            dma((1,)),
            dma((4, 4)),
            dma((1,)),
            dma((1,)),
            dma((1,)),
            dma((1,)),
            dma((1,)),
            dma((1,)),
        ],
        compiler_params=pltpu.CompilerParams(
            collective_id=0, has_side_effects=True, vmem_limit_bytes=60 * 1024 * 1024
        ),
        name="predict",
    )(
        token_ids,
        remask,
        mask_embed,
        gain_in.reshape(1, -1),
        gain_out.reshape(1, -1),
        table,
        w_qkv,
        w_out,
        position_embed,
    )
    log_probs, confidence, stats = pl.pallas_call(
        write_out,
        out_shape=(
            jax.ShapeDtypeStruct((1, 256, 256), BF),
            jax.ShapeDtypeStruct((1, 256), F32),
            jax.ShapeDtypeStruct((1, 2), F32),
        ),
        in_specs=[vmem] * 3,
        out_specs=(hbm, hbm, hbm),
        scratch_shapes=[dma((3,))],
        compiler_params=pltpu.CompilerParams(vmem_limit_bytes=1024 * 1024),
        name="write_out",
    )(log_probs, confidence, stats)
    return log_probs, confidence, stats.reshape(2)


def solution(mesh):
    finer = Mesh(mesh.devices.reshape(8, 4, 4, 2, 2), AXES)
    frames = ("clip", "zl", "x")
    tm = ("zl", "x")
    mp = ("zh", "core")
    in_specs = (
        P(frames, None),
        P(frames, None),
        P(tm, None, None),
        P(),
        P(mp, None),
        P(),
        P(),
        P(None, None, mp),
        P(mp, None),
    )
    out_specs = (P(frames, None, mp), P(frames, None), P("clip"))
    return jax.shard_map(body, mesh=finer, in_specs=in_specs, out_specs=out_specs, check_vma=False)
```

```python
import math

import jax
import jax.numpy as jnp
from jax import lax
from jax.experimental import pallas as pl
from jax.experimental.pallas import tpu as pltpu
from jax.sharding import Mesh
from jax.sharding import PartitionSpec as P

HEAD_DIM = 64
MESH = pl.DeviceIdType.MESH
AXES = ("clip", "zl", "x", "zh", "core")
BF = jnp.bfloat16
F32 = jnp.float32
SCALE = HEAD_DIM**-0.5 * math.log2(math.e)


def coords():
    return [lax.axis_index(name) for name in AXES]


def at(y, zl, x, zh, core):
    mine = coords()
    sizes = (8, 4, 4, 2, 2)
    return tuple(
        lax.rem(mine[k] + step + sizes[k], sizes[k]) if step else mine[k]
        for k, step in enumerate((y, zl, x, zh, core))
    )


def mirror():
    y, zl, x, zh, core = coords()
    return (y, 3 - zl, x, 1 - zh, core)


def remote(src, dst, send, recv, device):
    return pltpu.make_async_remote_copy(
        src_ref=src, dst_ref=dst, send_sem=send, recv_sem=recv, device_id=device, device_id_type=MESH
    )


def arrived(ref, sem):
    remote(ref, ref, sem, sem, at(0, 0, 0, 0, 1)).wait_recv()


def left(ref, sem):
    remote(ref, ref, sem, sem, at(0, 0, 0, 0, 1)).wait_send()


def norm_rows(h, gain):
    center = h - jnp.mean(h, axis=-1, keepdims=True)
    spread = jnp.mean(center * center, axis=-1, keepdims=True)
    return center * lax.rsqrt(spread + 1e-05) * gain


class Spread:
    def __init__(self, hbm, full, first, ssem, zsem, y1sem, x1sem, y2sem, x2sem, dsem):
        self.hbm, self.full, self.first, self.ssem, self.zsem, self.dsem = hbm, full, first, ssem, zsem, dsem
        self.y1, self.x1, self.y2, self.x2 = y1sem, x1sem, y2sem, x2sem
        y, zl, x, zh, core = coords()
        self.yq, self.x = lax.rem(y, 4), x
        self.own = zh * 2 + core
        self.got = (1 - zh) * 2 + core

    def quarter(self, k):
        return pl.ds(pl.multiple_of(k * 256, 256), 256)

    def rows(self, quarter, x):
        return pl.ds(pl.multiple_of(quarter * 256 + x * 64, 64), 64)

    def cols(self, yq, half):
        return pl.ds(pl.multiple_of(half * 512 + yq * 128, 128), 128)

    def piece(self, x, yq, half):
        return self.full.at[self.rows(self.got, x), self.cols(yq, half)]

    def strip(self, yq, half):
        return self.full.at[self.quarter(self.got), self.cols(yq, half)]

    def block(self, x):
        return self.full.at[self.rows(self.got, x), pl.ds(0, 512)]

    def y_of(self, dy):
        return lax.rem(self.yq - dy + 8, 4)

    def x_of(self, dx):
        return lax.rem(self.x - dx + 4, 4)

    def local(self):
        return pltpu.make_async_copy(self.hbm, self.full.at[self.quarter(self.own)], self.ssem.at[4])

    def fetch(self, half):
        rows = pl.ds(pl.multiple_of(self.x * 64, 64), 64)
        return pltpu.make_async_copy(
            self.hbm.at[rows, self.cols(self.yq, half)], self.first.at[half], self.ssem.at[5 + half]
        )

    def start_z(self):
        for half in range(2):
            piece = self.full.at[self.rows(self.own, self.x), self.cols(self.yq, half)]
            remote(self.first.at[half], piece, self.ssem.at[0], self.zsem.at[half], mirror()).start()

    def start_own_quarter(self):
        self.hand_over(self.full.at[self.quarter(self.own)], 0)

    def hand_over(self, ref, k):
        remote(ref, ref, self.ssem.at[3], self.dsem.at[k], at(0, 0, 0, 0, 1)).start()

    def along_y(self, ref, sem, recv):
        for dy in (2, 1, 7):
            remote(ref, ref, self.ssem.at[sem], recv.at[dy], at(dy, 0, 0, 0, 0)).start()

    def along_x(self, ref, sem, recv):
        for dx in (2, 1, 3):
            remote(ref, ref, self.ssem.at[sem], recv.at[dx], at(0, 0, dx, 0, 0)).start()

    def begin(self):
        first, second = self.piece(self.x, self.yq, 0), self.piece(self.x, self.yq, 1)
        arrived(first, self.zsem.at[0])
        self.along_y(first, 1, self.y1)
        arrived(second, self.zsem.at[1])
        self.along_x(second, 1, self.x1)
        self.along_x(first, 2, self.x2)
        self.along_y(second, 2, self.y2)

    def forward(self):
        for dy, dx in ((1, 1), (7, 3), (2, 2)):
            first = self.piece(self.x, self.y_of(dy), 0)
            arrived(first, self.y1.at[dy])
            self.along_x(first, 2, self.x2)
            second = self.piece(self.x_of(dx), self.yq, 1)
            arrived(second, self.x1.at[dx])
            self.along_y(second, 2, self.y2)
        self.hand_over(self.block(self.x), 1)
        self.hand_over(self.strip(self.yq, 1), 1)

    def finish(self):
        for dy, dx in ((1, 1), (7, 3), (2, 2)):
            block = self.block(self.x_of(dx))
            arrived(block, self.x2.at[dx])
            self.hand_over(block, 1)
            strip = self.strip(self.y_of(dy), 1)
            arrived(strip, self.y2.at[dy])
            self.hand_over(strip, 1)

    def wait_sent(self):
        left(self.full.at[pl.ds(0, 64), pl.ds(0, 256)], self.ssem.at[0])
        left(self.full.at[pl.ds(0, 64), pl.ds(0, 768)], self.ssem.at[1])
        left(self.full.at[pl.ds(0, 192)], self.ssem.at[2])
        left(self.full.at[pl.ds(0, 512)], self.ssem.at[3])

    def begin_slow(self):
        for half in range(2):
            piece = self.piece(self.x, self.yq, half)
            arrived(piece, self.zsem.at[half])
            self.along_x(piece, 1, self.x1)

    def forward_slow(self):
        for dx in (1, 3, 2):
            arrived(self.full.at[self.rows(self.got, self.x_of(dx)), pl.ds(0, 256)], self.x1.at[dx])
        for half in range(2):
            self.along_y(self.strip(self.yq, half), 2, self.y2)

    def finish_slow(self):
        for dy in (1, 7, 2):
            arrived(self.full.at[self.quarter(self.got), pl.ds(0, 256)], self.y2.at[dy])
        self.hand_over(self.full.at[self.quarter(self.got)], 1)

    def wait_sent_slow(self):
        left(self.full.at[pl.ds(0, 64), pl.ds(0, 256)], self.ssem.at[0])
        left(self.full.at[pl.ds(0, 64), pl.ds(0, 768)], self.ssem.at[1])
        left(self.full.at[pl.ds(0, 256), pl.ds(0, 768)], self.ssem.at[2])
        left(self.full.at[pl.ds(0, 512)], self.ssem.at[3])

    def wait_all(self):
        quarter = self.full.at[pl.ds(0, 256)]
        arrived(quarter, self.dsem.at[0])
        arrived(quarter, self.dsem.at[1])


def kernel(
    ids_hbm, remask_hbm, mask_hbm, gain_in_hbm, gain_out_hbm, table_hbm, wqkv_hbm, wout_hbm, pos_hbm,
    logp_ref, conf_ref, stats_ref,
    ids_ref, remask_ref, mask_embed_ref, gain_in_ref, gain_out_ref,
    table_first, wout_first, flipped, table, wout, wqkv, pos, hidden, normed, kv_out, q_out, kv, q_in, qpad, high, total, summed, o_out, ctx,
    final, logits, weight, stat_out, stat_in,
    local_sem, small_sem,
    t_s, t_z, t_y1, t_x1, t_y2, t_x2, t_d, w_s, w_z, w_y1, w_x1, w_y2, w_x2, w_d,
    a_send, a_recv, q_recv, b_send, b_recv,
    c_send, c_recv, f_send, f_recv, s_send, s_recv,
):
    y, zl, x, zh, core = coords()
    mp = zh * 2 + core
    frame = zl * 4 + x
    pair_z = (zl, zl + 1 - 2 * lax.rem(zl, 2), lax.rem(zl + 2, 4), 3 - zl)
    tab = Spread(table_hbm, table, table_first, t_s, t_z, t_y1, t_x1, t_y2, t_x2, t_d)
    out = Spread(wout_hbm, wout, wout_first, w_s, w_z, w_y1, w_x1, w_y2, w_x2, w_d)
    load_pos = pltpu.make_async_copy(pos_hbm.at[0], pos, local_sem.at[0])
    load_qkv = pltpu.make_async_copy(wqkv_hbm, wqkv, local_sem.at[1])

    small = [
        pltpu.make_async_copy(src, dst, small_sem.at[k])
        for k, (src, dst) in enumerate(
            (
                (ids_hbm, ids_ref),
                (remask_hbm, remask_ref),
                (mask_hbm, mask_embed_ref),
                (gain_in_hbm, gain_in_ref),
                (gain_out_hbm, gain_out_ref),
            )
        )
    ]
    for half in range(2):
        tab.fetch(half).start()
    barrier = pltpu.get_barrier_semaphore()
    peers = []
    for k in range(1, 16):
        place = lax.rem(zh * 8 + zl * 2 + core + k, 16)
        peers.append((y, lax.rem(place // 2, 4), x, place // 8, lax.rem(place, 2)))
    peers += [at(k, 0, 0, 0, 0) for k in (1, 2, 6, 7)]
    peers += [at(0, dz, dx, 0, dc) for dx in range(1, 4) for dz in range(4) for dc in range(2)]
    for peer in peers:
        pl.semaphore_signal(barrier, inc=1, device_id=peer, device_id_type=MESH)
    tab.local().start()
    for copy in small:
        copy.start()
    load_pos.start()
    out.local().start()
    for half in range(2):
        out.fetch(half).start()
    load_qkv.start()
    for half in range(2):
        tab.fetch(half).wait()
    pl.semaphore_wait(barrier, len(peers))
    tab.start_z()
    tab.local().wait()
    tab.start_own_quarter()
    for copy in small:
        copy.wait()
    row = lax.broadcasted_iota(jnp.int32, (256, 256), 0)
    lane = lax.broadcasted_iota(jnp.int32, (256, 256), 1)
    masked = jnp.max(jnp.where(remask_ref[...] == row, 1.0, 0.0), axis=1, keepdims=True)
    ids_col = jnp.sum(
        jnp.where(row == lane, ids_ref[...].astype(F32), 0.0), axis=1, keepdims=True
    )
    weight[...] = jnp.broadcast_to(masked, (256, 128))
    ids_col = jnp.where(masked > 0.5, -1.0, ids_col)
    mask_row = mask_embed_ref[...].astype(F32).reshape(1, 1024)

    def looked_up(first, count):
        entry = lax.broadcasted_iota(jnp.int32, (256, count), 1) + first
        onehot = jnp.where(entry.astype(F32) == ids_col, 1.0, 0.0).astype(BF)
        rows = table[pl.ds(pl.multiple_of(first, count), count)]
        return jnp.dot(onehot, rows, preferred_element_type=F32)

    load_pos.wait()
    for k in range(4):
        block = slice(k * 64, k * 64 + 64)
        hidden[block] = pos[block].astype(F32) + jnp.where(masked[block] > 0.5, mask_row, 0.0)
    tab.begin()
    for half in range(2):
        out.fetch(half).wait()
    out.start_z()
    arrived(table.at[pl.ds(0, 256)], tab.dsem.at[0])
    hidden[...] += looked_up(zh * 512, 512)
    tab.forward()
    out.begin_slow()
    tab.finish()
    out.forward_slow()
    out.local().wait()
    out.start_own_quarter()
    load_qkv.wait()
    hidden[...] += looked_up((2 - 2 * zh + core) * 256, 256)
    arrived(table.at[pl.ds(0, 256)], tab.dsem.at[1])
    hidden[...] += looked_up((3 - 2 * zh - core) * 256, 256)
    gain_in = gain_in_ref[...]
    for k in range(4):
        block = slice(k * 64, k * 64 + 64)
        normed[block] = norm_rows(hidden[block], gain_in).astype(BF)
    low = lax.broadcasted_iota(jnp.int32, (256, 128), 1) < 64
    n_all = normed[...]
    keys = jnp.dot(n_all, wqkv[1], preferred_element_type=F32)
    values = jnp.dot(n_all, wqkv[2], preferred_element_type=F32)
    for g in range(2):
        kg, vg = keys[:, g * 128 : g * 128 + 128], values[:, g * 128 : g * 128 + 128]
        kv_out[2 * g] = jnp.where(low, kg, pltpu.roll(vg, 64, 1)).astype(BF)
        kv_out[2 * g + 1] = jnp.where(low, pltpu.roll(kg, 64, 1), vg).astype(BF)
    query = jnp.dot(n_all, wqkv[0], preferred_element_type=F32)
    def spot(s, slot):
        return (0, 2, 1, 3)[s] * 4 + slot

    chunk = {0: slice(0, 4), 2: slice(4, 8), 1: slice(8, 13), 3: slice(13, 16)}

    def pass_on(block, s):
        for dx in (2, 1, 3):
            slot = (0, 1, 3, 2)[dx]
            remote(block, kv.at[spot(s, slot)], b_send.at[0], b_recv.at[s, slot], at(0, 0, dx, 0, 0)).start()

    pass_on(kv_out.at[zl], 0)
    def send_keys(d):
        remote(
            kv_out.at[pair_z[d]], kv.at[spot(d, 0)], a_send.at[0], a_recv.at[d], (y, pair_z[d], x, zh, core)
        ).start()

    def send_query(d):
        remote(
            q_out.at[pair_z[d]], q_in.at[d], a_send.at[1], q_recv.at[d], (y, pair_z[d], x, zh, core)
        ).start()

    send_keys(2)
    send_keys(1)
    low_half = low[:128]
    for g in range(2):
        qa, qb = query[:128, g * 128 : g * 128 + 128], query[128:, g * 128 : g * 128 + 128]
        q_out[2 * g] = jnp.where(low_half, qa, pltpu.roll(qb, 64, 1)).astype(BF)
        q_out[2 * g + 1] = jnp.where(low_half, pltpu.roll(qa, 64, 1), qb).astype(BF)
    send_query(1)
    send_query(2)
    send_keys(3)
    send_query(3)
    kv[spot(0, 0)] = kv_out[zl]

    def unpack(k, packed):
        packed = packed.astype(F32)
        qpad[k, :128] = jnp.where(low_half, packed, 0.0).astype(BF)
        qpad[k, 128:] = jnp.where(low_half, pltpu.roll(packed, 64, 1), 0.0).astype(BF)

    unpack(0, q_out[zl])
    low64 = low[:64]
    head_here = mp * 4 + zl

    def take(s):
        arrived(kv.at[spot(s, 0)], a_recv.at[s])
        pass_on(kv.at[spot(s, 0)], s)

    held = set()

    def ready(s, b):
        if b and (b, "q") not in held:
            arrived(q_in.at[b], q_recv.at[b])
            unpack(b, q_in[b])
            held.add((b, "q"))
        if s not in held:
            for slot in (1, 2, 3):
                arrived(kv.at[spot(s, slot)], b_recv.at[s, slot])
            held.add(s)

    def score(s, b):
        return lax.dot_general(
            qpad[b], kv[chunk[s]].reshape(-1, 128), (((1,), (1,)), ((), ())), preferred_element_type=F32
        )

    def absorb(s, b, scores):
        rows = kv[chunk[s]].reshape(-1, 128)
        top = jnp.max(scores, axis=1, keepdims=True)
        if s == 0:
            w = jnp.exp2(scores * SCALE - top * SCALE)
            high[b] = jnp.broadcast_to(top, (256, 128))
            total[b] = jnp.broadcast_to(jnp.sum(w, axis=1, keepdims=True), (256, 128))
            summed[b] = jnp.dot(w.astype(BF), rows, preferred_element_type=F32)
            return
        before = high[b]
        now = jnp.maximum(before, top)
        fade = jnp.exp2((before - now) * SCALE)
        w = jnp.exp2(scores * SCALE - now[:, :1] * SCALE)
        sums = total[b] * fade + jnp.sum(w, axis=1, keepdims=True)
        acc = summed[b] * fade + jnp.dot(w.astype(BF), rows, preferred_element_type=F32)
        if s != 3:
            high[b], total[b], summed[b] = now, sums, acc
            return
        rows = acc / sums
        for half in range(2):
            top_rows = rows[half * 128 : half * 128 + 64]
            low_rows = rows[half * 128 + 64 : half * 128 + 128]
            o_out[b, half] = jnp.where(low64, pltpu.roll(top_rows, 64, 1), low_rows).astype(BF)

    def send_context(b):
        for dh in (1, 0):
            for dc in (0, 1):
                if b == 0 and dh == 0 and dc == 0:
                    continue
                half = lax.rem(core + dc, 2)
                there = (y, pair_z[b], x, lax.rem(zh + dh, 2), half)
                remote(
                    o_out.at[b, half], ctx.at[head_here], c_send.at[0], c_recv.at[0], there
                ).start()

    steps = [(s, b) for s in (0, 2) for b in (0, 1, 2)] + [(0, 3), (2, 3)]
    steps += [(s, b) for s in (1, 3) for b in (2, 3, 1, 0)]
    take(2)
    take(1)
    ready(0, 0)
    scores = score(0, 0)
    for i, (s, b) in enumerate(steps):
        if i + 1 < len(steps):
            if steps[i + 1] == (2, 0):
                take(3)
            ready(*steps[i + 1])
            following = score(*steps[i + 1])
        absorb(s, b, scores)
        if s == 3:
            send_context(b)
        scores = following
    ctx[head_here] = o_out[0, core]
    out.finish_slow()
    for q in range(4):
        flipped[:, q * 256 : q * 256 + 256] = table[q * 256 : q * 256 + 256].T
    out.wait_all()

    arrived(ctx.at[pl.ds(0, 15)], c_recv.at[0])
    pieces = []
    for g in range(8):
        a, b = ctx[2 * g].astype(F32), ctx[2 * g + 1].astype(F32)
        pieces.append(
            jnp.concatenate(
                [
                    jnp.where(low64, a, pltpu.roll(b, 64, 1)),
                    jnp.where(low64, pltpu.roll(a, 64, 1), b),
                ],
                axis=0,
            ).astype(BF)
        )
    context = jnp.concatenate(pieces, axis=1)
    mine = pl.ds(pl.multiple_of(core * 128, 128), 128)
    h = hidden[mine] + jnp.dot(context, wout[...], preferred_element_type=F32)
    final[mine] = norm_rows(h, gain_out_ref[...]).astype(BF)
    send_final = remote(final.at[mine], final.at[mine], f_send.at[0], f_recv.at[0], at(0, 0, 0, 0, 1))
    send_final.start()

    def finish(block):
        rows = final[block]
        tops = []
        for q in range(4):
            part = jnp.dot(rows, flipped[:, q * 256 : q * 256 + 256], preferred_element_type=F32)
            logits[q, block] = part
            tops.append(jnp.max(part, axis=1, keepdims=True))
        top = jnp.maximum(jnp.maximum(tops[0], tops[1]), jnp.maximum(tops[2], tops[3]))
        sums = jnp.zeros_like(top)
        for q in range(4):
            sums = sums + jnp.sum(jnp.exp(logits[q, block] - top), axis=1, keepdims=True)
        lse = top + jnp.log(sums)
        conf = jnp.exp(top - lse)
        high[0, block] = jnp.broadcast_to(conf, (128, 128))
        return conf, lse

    def put_rows(block, lse):
        logp_ref[block] = (logits[mp, block] - lse).astype(BF)

    conf, lse = finish(mine)
    w = weight[mine][:, :1]
    lane1 = lax.broadcasted_iota(jnp.int32, (1, 128), 1)
    conf_sum = jnp.sum(conf * w, axis=0, keepdims=True)
    count = jnp.sum(w, axis=0, keepdims=True)
    tile = jnp.where(lane1 == 0, conf_sum, jnp.where(lane1 == 1, count, 0.0))
    place = frame * 2 + core
    stat_out[...] = tile
    stat_in[place] = tile
    for dz in (2, 3, 1, 0):
        for dx in (2, 3, 1, 0):
            for dc in range(2):
                if dz or dx or dc:
                    remote(
                        stat_out, stat_in.at[place], s_send.at[0], s_recv.at[0], at(0, dz, dx, 0, dc)
                    ).start()
    put_rows(mine, lse)
    other = pl.ds(pl.multiple_of((1 - core) * 128, 128), 128)
    arrived(final.at[other], f_recv.at[0])
    conf, lse = finish(other)
    put_rows(other, lse)
    conf_ref[...] = jnp.sum(jnp.where(row == lane, high[0][:, :1], 0.0), axis=0, keepdims=True)
    tab.wait_sent()
    out.wait_sent_slow()
    left(kv_out.at[pl.ds(0, 3)], a_send.at[0])
    left(q_out.at[pl.ds(0, 3)], a_send.at[1])
    left(kv.at[pl.ds(0, 12)], b_send.at[0])
    left(ctx.at[pl.ds(0, 15)], c_send.at[0])
    send_final.wait_send()
    arrived(stat_in.at[pl.ds(0, 31)], s_recv.at[0])
    left(stat_in.at[pl.ds(0, 31)], s_send.at[0])
    sums = stat_in[0]
    for k in range(1, 32):
        sums = sums + stat_in[k]
    all_conf = jnp.sum(jnp.where(lane1 == 0, sums, 0.0), axis=1, keepdims=True)
    all_count = jnp.sum(jnp.where(lane1 == 1, sums, 0.0), axis=1, keepdims=True)
    both = jnp.where(lane1 == 0, all_conf / all_count, jnp.log(all_count / 4096.0))
    stats_ref[...] = both[:, :2]


def write_out(logp, conf, stats, logp_out, conf_out, stats_out, sem):
    copies = [
        pltpu.make_async_copy(src, dst, sem.at[k])
        for k, (src, dst) in enumerate(((logp, logp_out.at[0]), (conf, conf_out), (stats, stats_out)))
    ]
    for copy in copies:
        copy.start()
    for copy in copies:
        copy.wait()


def body(token_ids, remask, position_embed, mask_embed, table, gain_in, gain_out, w_qkv, w_out):
    vmem = pl.BlockSpec(memory_space=pltpu.VMEM)
    hbm = pl.BlockSpec(memory_space=pl.ANY)
    dma = pltpu.SemaphoreType.DMA
    spread_sems = [dma((7,)), dma((2,)), dma((8,)), dma((4,)), dma((8,)), dma((4,)), dma((2,))]
    log_probs, confidence, stats = pl.pallas_call(
        kernel,
        out_shape=(
            pltpu.VMEM((256, 256), BF),
            pltpu.VMEM((1, 256), F32),
            pltpu.VMEM((1, 2), F32),
        ),
        in_specs=[hbm] * 9,
        out_specs=(vmem, vmem, vmem),
        scratch_shapes=[
            pltpu.VMEM((1, 256), jnp.int32),
            pltpu.VMEM((1, 256), jnp.int32),
            pltpu.VMEM((1024,), BF),
            pltpu.VMEM((1, 1024), F32),
            pltpu.VMEM((1, 1024), F32),
            pltpu.VMEM((2, 64, 128), BF),
            pltpu.VMEM((2, 64, 128), BF),
            pltpu.VMEM((1024, 1024), BF),
            pltpu.VMEM((1024, 1024), BF),
            pltpu.VMEM((1024, 1024), BF),
            pltpu.VMEM((3, 1024, 256), BF),
            pltpu.VMEM((256, 1024), BF),
            pltpu.VMEM((256, 1024), F32),
            pltpu.VMEM((256, 1024), BF),
            pltpu.VMEM((4, 256, 128), BF),
            pltpu.VMEM((4, 128, 128), BF),
            pltpu.VMEM((16, 256, 128), BF),
            pltpu.VMEM((4, 128, 128), BF),
            pltpu.VMEM((4, 256, 128), BF),
            pltpu.VMEM((4, 256, 128), F32),
            pltpu.VMEM((4, 256, 128), F32),
            pltpu.VMEM((4, 256, 128), F32),
            pltpu.VMEM((4, 2, 64, 128), BF),
            pltpu.VMEM((16, 64, 128), BF),
            pltpu.VMEM((256, 1024), BF),
            pltpu.VMEM((4, 256, 256), F32),
            pltpu.VMEM((256, 128), F32),
            pltpu.VMEM((1, 128), F32),
            pltpu.VMEM((32, 1, 128), F32),
            dma((2,)),
            dma((5,)),
            *spread_sems,
            *spread_sems,
            dma((2,)),
            dma((4,)),
            dma((4,)),
            dma((1,)),
            dma((4, 4)),
            dma((1,)),
            dma((1,)),
            dma((1,)),
            dma((1,)),
            dma((1,)),
            dma((1,)),
        ],
        compiler_params=pltpu.CompilerParams(
            collective_id=0, has_side_effects=True, vmem_limit_bytes=60 * 1024 * 1024
        ),
        name="predict",
    )(
        token_ids,
        remask,
        mask_embed,
        gain_in.reshape(1, -1),
        gain_out.reshape(1, -1),
        table,
        w_qkv,
        w_out,
        position_embed,
    )
    log_probs, confidence, stats = pl.pallas_call(
        write_out,
        out_shape=(
            jax.ShapeDtypeStruct((1, 256, 256), BF),
            jax.ShapeDtypeStruct((1, 256), F32),
            jax.ShapeDtypeStruct((1, 2), F32),
        ),
        in_specs=[vmem] * 3,
        out_specs=(hbm, hbm, hbm),
        scratch_shapes=[dma((3,))],
        compiler_params=pltpu.CompilerParams(vmem_limit_bytes=1024 * 1024),
        name="write_out",
    )(log_probs, confidence, stats)
    return log_probs, confidence, stats.reshape(2)


def solution(mesh):
    finer = Mesh(mesh.devices.reshape(8, 4, 4, 2, 2), AXES)
    frames = ("clip", "zl", "x")
    tm = ("zl", "x")
    mp = ("zh", "core")
    in_specs = (
        P(frames, None),
        P(frames, None),
        P(tm, None, None),
        P(),
        P(mp, None),
        P(),
        P(),
        P(None, None, mp),
        P(mp, None),
    )
    out_specs = (P(frames, None, mp), P(frames, None), P("clip"))
    return jax.shard_map(body, mesh=finer, in_specs=in_specs, out_specs=out_specs, check_vma=False)
```

```python
import math

import jax
import jax.numpy as jnp
from jax import lax
from jax.experimental import pallas as pl
from jax.experimental.pallas import tpu as pltpu
from jax.sharding import Mesh
from jax.sharding import PartitionSpec as P

HEAD_DIM = 64
MESH = pl.DeviceIdType.MESH
AXES = ("clip", "zl", "x", "zh", "core")
BF = jnp.bfloat16
F32 = jnp.float32
SCALE = HEAD_DIM**-0.5 * math.log2(math.e)


def coords():
    return [lax.axis_index(name) for name in AXES]


def at(y, zl, x, zh, core):
    mine = coords()
    sizes = (8, 4, 4, 2, 2)
    return tuple(
        lax.rem(mine[k] + step + sizes[k], sizes[k]) if step else mine[k]
        for k, step in enumerate((y, zl, x, zh, core))
    )


def mirror():
    y, zl, x, zh, core = coords()
    return (y, 3 - zl, x, 1 - zh, core)


def remote(src, dst, send, recv, device):
    return pltpu.make_async_remote_copy(
        src_ref=src, dst_ref=dst, send_sem=send, recv_sem=recv, device_id=device, device_id_type=MESH
    )


def arrived(ref, sem):
    remote(ref, ref, sem, sem, at(0, 0, 0, 0, 1)).wait_recv()


def left(ref, sem):
    remote(ref, ref, sem, sem, at(0, 0, 0, 0, 1)).wait_send()


def norm_rows(h, gain):
    center = h - jnp.mean(h, axis=-1, keepdims=True)
    spread = jnp.mean(center * center, axis=-1, keepdims=True)
    return center * lax.rsqrt(spread + 1e-05) * gain


class Spread:
    def __init__(self, hbm, full, first, ssem, zsem, y1sem, x1sem, y2sem, x2sem, dsem):
        self.hbm, self.full, self.first, self.ssem, self.zsem, self.dsem = hbm, full, first, ssem, zsem, dsem
        self.y1, self.x1, self.y2, self.x2 = y1sem, x1sem, y2sem, x2sem
        y, zl, x, zh, core = coords()
        self.yq, self.x = lax.rem(y, 4), x
        self.own = zh * 2 + core
        self.got = (1 - zh) * 2 + core

    def quarter(self, k):
        return pl.ds(pl.multiple_of(k * 256, 256), 256)

    def rows(self, quarter, x):
        return pl.ds(pl.multiple_of(quarter * 256 + x * 64, 64), 64)

    def cols(self, yq, half):
        return pl.ds(pl.multiple_of(half * 512 + yq * 128, 128), 128)

    def piece(self, x, yq, half):
        return self.full.at[self.rows(self.got, x), self.cols(yq, half)]

    def strip(self, yq, half):
        return self.full.at[self.quarter(self.got), self.cols(yq, half)]

    def block(self, x):
        return self.full.at[self.rows(self.got, x), pl.ds(0, 512)]

    def y_of(self, dy):
        return lax.rem(self.yq - dy + 8, 4)

    def x_of(self, dx):
        return lax.rem(self.x - dx + 4, 4)

    def local(self):
        return pltpu.make_async_copy(self.hbm, self.full.at[self.quarter(self.own)], self.ssem.at[4])

    def fetch(self, half):
        rows = pl.ds(pl.multiple_of(self.x * 64, 64), 64)
        return pltpu.make_async_copy(
            self.hbm.at[rows, self.cols(self.yq, half)], self.first.at[half], self.ssem.at[5 + half]
        )

    def start_z(self):
        for half in range(2):
            piece = self.full.at[self.rows(self.own, self.x), self.cols(self.yq, half)]
            remote(self.first.at[half], piece, self.ssem.at[0], self.zsem.at[half], mirror()).start()

    def start_own_quarter(self):
        self.hand_over(self.full.at[self.quarter(self.own)], 0)

    def hand_over(self, ref, k):
        remote(ref, ref, self.ssem.at[3], self.dsem.at[k], at(0, 0, 0, 0, 1)).start()

    def along_y(self, ref, sem, recv):
        for dy in (2, 1, 7):
            remote(ref, ref, self.ssem.at[sem], recv.at[dy], at(dy, 0, 0, 0, 0)).start()

    def along_x(self, ref, sem, recv):
        for dx in (2, 1, 3):
            remote(ref, ref, self.ssem.at[sem], recv.at[dx], at(0, 0, dx, 0, 0)).start()

    def begin(self):
        first, second = self.piece(self.x, self.yq, 0), self.piece(self.x, self.yq, 1)
        arrived(first, self.zsem.at[0])
        self.along_y(first, 1, self.y1)
        arrived(second, self.zsem.at[1])
        self.along_x(second, 1, self.x1)
        self.along_x(first, 2, self.x2)
        self.along_y(second, 2, self.y2)

    def forward(self):
        for dy, dx in ((1, 1), (7, 3), (2, 2)):
            first = self.piece(self.x, self.y_of(dy), 0)
            arrived(first, self.y1.at[dy])
            self.along_x(first, 2, self.x2)
            second = self.piece(self.x_of(dx), self.yq, 1)
            arrived(second, self.x1.at[dx])
            self.along_y(second, 2, self.y2)
        self.hand_over(self.block(self.x), 1)
        self.hand_over(self.strip(self.yq, 1), 1)

    def finish(self):
        for dy, dx in ((1, 1), (7, 3), (2, 2)):
            block = self.block(self.x_of(dx))
            arrived(block, self.x2.at[dx])
            self.hand_over(block, 1)
            strip = self.strip(self.y_of(dy), 1)
            arrived(strip, self.y2.at[dy])
            self.hand_over(strip, 1)

    def wait_sent(self):
        left(self.full.at[pl.ds(0, 64), pl.ds(0, 256)], self.ssem.at[0])
        left(self.full.at[pl.ds(0, 64), pl.ds(0, 768)], self.ssem.at[1])
        left(self.full.at[pl.ds(0, 192)], self.ssem.at[2])
        left(self.full.at[pl.ds(0, 512)], self.ssem.at[3])

    def begin_slow(self):
        for half in range(2):
            piece = self.piece(self.x, self.yq, half)
            arrived(piece, self.zsem.at[half])
            self.along_x(piece, 1, self.x1)

    def forward_slow(self):
        for dx in (1, 3, 2):
            arrived(self.full.at[self.rows(self.got, self.x_of(dx)), pl.ds(0, 256)], self.x1.at[dx])
        for half in range(2):
            self.along_y(self.strip(self.yq, half), 2, self.y2)

    def finish_slow(self):
        for dy in (1, 7, 2):
            arrived(self.full.at[self.quarter(self.got), pl.ds(0, 256)], self.y2.at[dy])
        self.hand_over(self.full.at[self.quarter(self.got)], 1)

    def wait_sent_slow(self):
        left(self.full.at[pl.ds(0, 64), pl.ds(0, 256)], self.ssem.at[0])
        left(self.full.at[pl.ds(0, 64), pl.ds(0, 768)], self.ssem.at[1])
        left(self.full.at[pl.ds(0, 256), pl.ds(0, 768)], self.ssem.at[2])
        left(self.full.at[pl.ds(0, 512)], self.ssem.at[3])

    def wait_all(self):
        quarter = self.full.at[pl.ds(0, 256)]
        arrived(quarter, self.dsem.at[0])
        arrived(quarter, self.dsem.at[1])


def kernel(
    ids_hbm, remask_hbm, mask_hbm, gain_in_hbm, gain_out_hbm, table_hbm, wqkv_hbm, wout_hbm, pos_hbm,
    logp_ref, conf_ref, stats_ref,
    ids_ref, remask_ref, mask_embed_ref, gain_in_ref, gain_out_ref,
    table_first, wout_first, flipped, table, wout, wqkv, pos, hidden, normed, kv_out, q_out, kv, q_in, qpad, high, total, summed, o_out, ctx,
    final, logits, weight, stat_out, stat_in,
    local_sem, small_sem,
    t_s, t_z, t_y1, t_x1, t_y2, t_x2, t_d, w_s, w_z, w_y1, w_x1, w_y2, w_x2, w_d,
    a_send, a_recv, q_recv, b_send, b_recv,
    c_send, c_recv, f_send, f_recv, s_send, s_recv,
):
    y, zl, x, zh, core = coords()
    mp = zh * 2 + core
    frame = zl * 4 + x
    pair_z = (zl, zl + 1 - 2 * lax.rem(zl, 2), lax.rem(zl + 2, 4), 3 - zl)
    tab = Spread(table_hbm, table, table_first, t_s, t_z, t_y1, t_x1, t_y2, t_x2, t_d)
    out = Spread(wout_hbm, wout, wout_first, w_s, w_z, w_y1, w_x1, w_y2, w_x2, w_d)
    load_pos = pltpu.make_async_copy(pos_hbm.at[0], pos, local_sem.at[0])
    load_qkv = pltpu.make_async_copy(wqkv_hbm, wqkv, local_sem.at[1])

    small = [
        pltpu.make_async_copy(src, dst, small_sem.at[k])
        for k, (src, dst) in enumerate(
            (
                (ids_hbm, ids_ref),
                (remask_hbm, remask_ref),
                (mask_hbm, mask_embed_ref),
                (gain_in_hbm, gain_in_ref),
                (gain_out_hbm, gain_out_ref),
            )
        )
    ]
    for half in range(2):
        tab.fetch(half).start()
    barrier = pltpu.get_barrier_semaphore()
    peers = []
    for k in range(1, 16):
        place = lax.rem(zh * 8 + zl * 2 + core + k, 16)
        peers.append((y, lax.rem(place // 2, 4), x, place // 8, lax.rem(place, 2)))
    peers += [at(k, 0, 0, 0, 0) for k in (1, 2, 6, 7)]
    peers += [at(0, dz, dx, 0, dc) for dx in range(1, 4) for dz in range(4) for dc in range(2)]
    for peer in peers:
        pl.semaphore_signal(barrier, inc=1, device_id=peer, device_id_type=MESH)
    tab.local().start()
    for copy in small:
        copy.start()
    load_pos.start()
    out.local().start()
    for half in range(2):
        out.fetch(half).start()
    load_qkv.start()
    for half in range(2):
        tab.fetch(half).wait()
    pl.semaphore_wait(barrier, len(peers))
    tab.start_z()
    tab.local().wait()
    tab.start_own_quarter()
    for copy in small:
        copy.wait()
    row = lax.broadcasted_iota(jnp.int32, (256, 256), 0)
    lane = lax.broadcasted_iota(jnp.int32, (256, 256), 1)
    masked = jnp.max(jnp.where(remask_ref[...] == row, 1.0, 0.0), axis=1, keepdims=True)
    ids_col = jnp.sum(
        jnp.where(row == lane, ids_ref[...].astype(F32), 0.0), axis=1, keepdims=True
    )
    weight[...] = jnp.broadcast_to(masked, (256, 128))
    ids_col = jnp.where(masked > 0.5, -1.0, ids_col)
    mask_row = mask_embed_ref[...].astype(F32).reshape(1, 1024)

    def looked_up(first, count):
        entry = lax.broadcasted_iota(jnp.int32, (256, count), 1) + first
        onehot = jnp.where(entry.astype(F32) == ids_col, 1.0, 0.0).astype(BF)
        rows = table[pl.ds(pl.multiple_of(first, count), count)]
        return jnp.dot(onehot, rows, preferred_element_type=F32)

    load_pos.wait()
    for k in range(4):
        block = slice(k * 64, k * 64 + 64)
        hidden[block] = pos[block].astype(F32) + jnp.where(masked[block] > 0.5, mask_row, 0.0)
    tab.begin()
    for half in range(2):
        out.fetch(half).wait()
    out.start_z()
    arrived(table.at[pl.ds(0, 256)], tab.dsem.at[0])
    hidden[...] += looked_up(zh * 512, 512)
    tab.forward()
    out.begin_slow()
    tab.finish()
    out.forward_slow()
    out.local().wait()
    out.start_own_quarter()
    load_qkv.wait()
    hidden[...] += looked_up((2 - 2 * zh + core) * 256, 256)
    arrived(table.at[pl.ds(0, 256)], tab.dsem.at[1])
    hidden[...] += looked_up((3 - 2 * zh - core) * 256, 256)
    gain_in = gain_in_ref[...]
    for k in range(4):
        block = slice(k * 64, k * 64 + 64)
        normed[block] = norm_rows(hidden[block], gain_in).astype(BF)
    low = lax.broadcasted_iota(jnp.int32, (256, 128), 1) < 64
    n_all = normed[...]
    keys = jnp.dot(n_all, wqkv[1], preferred_element_type=F32)
    values = jnp.dot(n_all, wqkv[2], preferred_element_type=F32)
    for g in range(2):
        kg, vg = keys[:, g * 128 : g * 128 + 128], values[:, g * 128 : g * 128 + 128]
        kv_out[2 * g] = jnp.where(low, kg, pltpu.roll(vg, 64, 1)).astype(BF)
        kv_out[2 * g + 1] = jnp.where(low, pltpu.roll(kg, 64, 1), vg).astype(BF)
    def spot(s, slot):
        return (0, 2, 1, 3)[s] * 4 + slot

    chunk = {0: slice(0, 4), 2: slice(4, 8), 1: slice(8, 13), 3: slice(13, 16)}

    def pass_on(block, s):
        for dx in (2, 1, 3):
            slot = (0, 1, 3, 2)[dx]
            remote(block, kv.at[spot(s, slot)], b_send.at[0], b_recv.at[s, slot], at(0, 0, dx, 0, 0)).start()

    pass_on(kv_out.at[zl], 0)
    def send_keys(d):
        remote(
            kv_out.at[pair_z[d]], kv.at[spot(d, 0)], a_send.at[0], a_recv.at[d], (y, pair_z[d], x, zh, core)
        ).start()

    def send_query(d):
        remote(
            q_out.at[pair_z[d]], q_in.at[d], a_send.at[1], q_recv.at[d], (y, pair_z[d], x, zh, core)
        ).start()

    send_keys(2)
    send_keys(1)
    query = jnp.dot(n_all, wqkv[0], preferred_element_type=F32)
    low_half = low[:128]
    for g in range(2):
        qa, qb = query[:128, g * 128 : g * 128 + 128], query[128:, g * 128 : g * 128 + 128]
        q_out[2 * g] = jnp.where(low_half, qa, pltpu.roll(qb, 64, 1)).astype(BF)
        q_out[2 * g + 1] = jnp.where(low_half, pltpu.roll(qa, 64, 1), qb).astype(BF)
    send_query(1)
    send_query(2)
    send_keys(3)
    send_query(3)
    kv[spot(0, 0)] = kv_out[zl]

    def unpack(k, packed):
        packed = packed.astype(F32)
        qpad[k, :128] = jnp.where(low_half, packed, 0.0).astype(BF)
        qpad[k, 128:] = jnp.where(low_half, pltpu.roll(packed, 64, 1), 0.0).astype(BF)

    unpack(0, q_out[zl])
    low64 = low[:64]
    head_here = mp * 4 + zl

    def take(s):
        arrived(kv.at[spot(s, 0)], a_recv.at[s])
        pass_on(kv.at[spot(s, 0)], s)

    held = set()

    def ready(s, b):
        if b and (b, "q") not in held:
            arrived(q_in.at[b], q_recv.at[b])
            unpack(b, q_in[b])
            held.add((b, "q"))
        if s not in held:
            for slot in (1, 2, 3):
                arrived(kv.at[spot(s, slot)], b_recv.at[s, slot])
            held.add(s)

    def score(s, b):
        return lax.dot_general(
            qpad[b], kv[chunk[s]].reshape(-1, 128), (((1,), (1,)), ((), ())), preferred_element_type=F32
        )

    def absorb(s, b, scores):
        rows = kv[chunk[s]].reshape(-1, 128)
        top = jnp.max(scores, axis=1, keepdims=True)
        if s == 0:
            w = jnp.exp2(scores * SCALE - top * SCALE)
            high[b] = jnp.broadcast_to(top, (256, 128))
            total[b] = jnp.broadcast_to(jnp.sum(w, axis=1, keepdims=True), (256, 128))
            summed[b] = jnp.dot(w.astype(BF), rows, preferred_element_type=F32)
            return
        before = high[b]
        now = jnp.maximum(before, top)
        fade = jnp.exp2((before - now) * SCALE)
        w = jnp.exp2(scores * SCALE - now[:, :1] * SCALE)
        sums = total[b] * fade + jnp.sum(w, axis=1, keepdims=True)
        acc = summed[b] * fade + jnp.dot(w.astype(BF), rows, preferred_element_type=F32)
        if s != 3:
            high[b], total[b], summed[b] = now, sums, acc
            return
        rows = acc / sums
        for half in range(2):
            top_rows = rows[half * 128 : half * 128 + 64]
            low_rows = rows[half * 128 + 64 : half * 128 + 128]
            o_out[b, half] = jnp.where(low64, pltpu.roll(top_rows, 64, 1), low_rows).astype(BF)

    def send_context(b):
        for dh in (1, 0):
            for dc in (0, 1):
                if b == 0 and dh == 0 and dc == 0:
                    continue
                half = lax.rem(core + dc, 2)
                there = (y, pair_z[b], x, lax.rem(zh + dh, 2), half)
                remote(
                    o_out.at[b, half], ctx.at[head_here], c_send.at[0], c_recv.at[0], there
                ).start()

    steps = [(s, b) for s in (0, 2) for b in (0, 1, 2)] + [(0, 3), (2, 3)]
    steps += [(s, b) for s in (1, 3) for b in (2, 3, 1, 0)]
    take(2)
    take(1)
    ready(0, 0)
    scores = score(0, 0)
    for i, (s, b) in enumerate(steps):
        if i + 1 < len(steps):
            if steps[i + 1] == (2, 0):
                take(3)
            ready(*steps[i + 1])
            following = score(*steps[i + 1])
        absorb(s, b, scores)
        if s == 3:
            send_context(b)
        scores = following
    ctx[head_here] = o_out[0, core]
    out.finish_slow()
    for q in range(4):
        flipped[:, q * 256 : q * 256 + 256] = table[q * 256 : q * 256 + 256].T
    out.wait_all()

    arrived(ctx.at[pl.ds(0, 15)], c_recv.at[0])
    pieces = []
    for g in range(8):
        a, b = ctx[2 * g].astype(F32), ctx[2 * g + 1].astype(F32)
        pieces.append(
            jnp.concatenate(
                [
                    jnp.where(low64, a, pltpu.roll(b, 64, 1)),
                    jnp.where(low64, pltpu.roll(a, 64, 1), b),
                ],
                axis=0,
            ).astype(BF)
        )
    context = jnp.concatenate(pieces, axis=1)
    mine = pl.ds(pl.multiple_of(core * 128, 128), 128)
    h = hidden[mine] + jnp.dot(context, wout[...], preferred_element_type=F32)
    final[mine] = norm_rows(h, gain_out_ref[...]).astype(BF)
    send_final = remote(final.at[mine], final.at[mine], f_send.at[0], f_recv.at[0], at(0, 0, 0, 0, 1))
    send_final.start()

    def finish(block):
        rows = final[block]
        tops = []
        for q in range(4):
            part = jnp.dot(rows, flipped[:, q * 256 : q * 256 + 256], preferred_element_type=F32)
            logits[q, block] = part
            tops.append(jnp.max(part, axis=1, keepdims=True))
        top = jnp.maximum(jnp.maximum(tops[0], tops[1]), jnp.maximum(tops[2], tops[3]))
        sums = jnp.zeros_like(top)
        for q in range(4):
            sums = sums + jnp.sum(jnp.exp(logits[q, block] - top), axis=1, keepdims=True)
        lse = top + jnp.log(sums)
        conf = jnp.exp(top - lse)
        high[0, block] = jnp.broadcast_to(conf, (128, 128))
        return conf, lse

    def put_rows(block, lse):
        logp_ref[block] = (logits[mp, block] - lse).astype(BF)

    conf, lse = finish(mine)
    w = weight[mine][:, :1]
    lane1 = lax.broadcasted_iota(jnp.int32, (1, 128), 1)
    conf_sum = jnp.sum(conf * w, axis=0, keepdims=True)
    count = jnp.sum(w, axis=0, keepdims=True)
    tile = jnp.where(lane1 == 0, conf_sum, jnp.where(lane1 == 1, count, 0.0))
    place = frame * 2 + core
    stat_out[...] = tile
    stat_in[place] = tile
    for dz in (2, 3, 1, 0):
        for dx in (2, 3, 1, 0):
            for dc in range(2):
                if dz or dx or dc:
                    remote(
                        stat_out, stat_in.at[place], s_send.at[0], s_recv.at[0], at(0, dz, dx, 0, dc)
                    ).start()
    put_rows(mine, lse)
    other = pl.ds(pl.multiple_of((1 - core) * 128, 128), 128)
    arrived(final.at[other], f_recv.at[0])
    conf, lse = finish(other)
    put_rows(other, lse)
    conf_ref[...] = jnp.sum(jnp.where(row == lane, high[0][:, :1], 0.0), axis=0, keepdims=True)
    tab.wait_sent()
    out.wait_sent_slow()
    left(kv_out.at[pl.ds(0, 3)], a_send.at[0])
    left(q_out.at[pl.ds(0, 3)], a_send.at[1])
    left(kv.at[pl.ds(0, 12)], b_send.at[0])
    left(ctx.at[pl.ds(0, 15)], c_send.at[0])
    send_final.wait_send()
    arrived(stat_in.at[pl.ds(0, 31)], s_recv.at[0])
    left(stat_in.at[pl.ds(0, 31)], s_send.at[0])
    sums = stat_in[0]
    for k in range(1, 32):
        sums = sums + stat_in[k]
    all_conf = jnp.sum(jnp.where(lane1 == 0, sums, 0.0), axis=1, keepdims=True)
    all_count = jnp.sum(jnp.where(lane1 == 1, sums, 0.0), axis=1, keepdims=True)
    both = jnp.where(lane1 == 0, all_conf / all_count, jnp.log(all_count / 4096.0))
    stats_ref[...] = both[:, :2]


def write_out(logp, conf, stats, logp_out, conf_out, stats_out, sem):
    copies = [
        pltpu.make_async_copy(src, dst, sem.at[k])
        for k, (src, dst) in enumerate(((logp, logp_out.at[0]), (conf, conf_out), (stats, stats_out)))
    ]
    for copy in copies:
        copy.start()
    for copy in copies:
        copy.wait()


def body(token_ids, remask, position_embed, mask_embed, table, gain_in, gain_out, w_qkv, w_out):
    vmem = pl.BlockSpec(memory_space=pltpu.VMEM)
    hbm = pl.BlockSpec(memory_space=pl.ANY)
    dma = pltpu.SemaphoreType.DMA
    spread_sems = [dma((7,)), dma((2,)), dma((8,)), dma((4,)), dma((8,)), dma((4,)), dma((2,))]
    log_probs, confidence, stats = pl.pallas_call(
        kernel,
        out_shape=(
            pltpu.VMEM((256, 256), BF),
            pltpu.VMEM((1, 256), F32),
            pltpu.VMEM((1, 2), F32),
        ),
        in_specs=[hbm] * 9,
        out_specs=(vmem, vmem, vmem),
        scratch_shapes=[
            pltpu.VMEM((1, 256), jnp.int32),
            pltpu.VMEM((1, 256), jnp.int32),
            pltpu.VMEM((1024,), BF),
            pltpu.VMEM((1, 1024), F32),
            pltpu.VMEM((1, 1024), F32),
            pltpu.VMEM((2, 64, 128), BF),
            pltpu.VMEM((2, 64, 128), BF),
            pltpu.VMEM((1024, 1024), BF),
            pltpu.VMEM((1024, 1024), BF),
            pltpu.VMEM((1024, 1024), BF),
            pltpu.VMEM((3, 1024, 256), BF),
            pltpu.VMEM((256, 1024), BF),
            pltpu.VMEM((256, 1024), F32),
            pltpu.VMEM((256, 1024), BF),
            pltpu.VMEM((4, 256, 128), BF),
            pltpu.VMEM((4, 128, 128), BF),
            pltpu.VMEM((16, 256, 128), BF),
            pltpu.VMEM((4, 128, 128), BF),
            pltpu.VMEM((4, 256, 128), BF),
            pltpu.VMEM((4, 256, 128), F32),
            pltpu.VMEM((4, 256, 128), F32),
            pltpu.VMEM((4, 256, 128), F32),
            pltpu.VMEM((4, 2, 64, 128), BF),
            pltpu.VMEM((16, 64, 128), BF),
            pltpu.VMEM((256, 1024), BF),
            pltpu.VMEM((4, 256, 256), F32),
            pltpu.VMEM((256, 128), F32),
            pltpu.VMEM((1, 128), F32),
            pltpu.VMEM((32, 1, 128), F32),
            dma((2,)),
            dma((5,)),
            *spread_sems,
            *spread_sems,
            dma((2,)),
            dma((4,)),
            dma((4,)),
            dma((1,)),
            dma((4, 4)),
            dma((1,)),
            dma((1,)),
            dma((1,)),
            dma((1,)),
            dma((1,)),
            dma((1,)),
        ],
        compiler_params=pltpu.CompilerParams(
            collective_id=0, has_side_effects=True, vmem_limit_bytes=60 * 1024 * 1024
        ),
        name="predict",
    )(
        token_ids,
        remask,
        mask_embed,
        gain_in.reshape(1, -1),
        gain_out.reshape(1, -1),
        table,
        w_qkv,
        w_out,
        position_embed,
    )
    log_probs, confidence, stats = pl.pallas_call(
        write_out,
        out_shape=(
            jax.ShapeDtypeStruct((1, 256, 256), BF),
            jax.ShapeDtypeStruct((1, 256), F32),
            jax.ShapeDtypeStruct((1, 2), F32),
        ),
        in_specs=[vmem] * 3,
        out_specs=(hbm, hbm, hbm),
        scratch_shapes=[dma((3,))],
        compiler_params=pltpu.CompilerParams(vmem_limit_bytes=1024 * 1024),
        name="write_out",
    )(log_probs, confidence, stats)
    return log_probs, confidence, stats.reshape(2)


def solution(mesh):
    finer = Mesh(mesh.devices.reshape(8, 4, 4, 2, 2), AXES)
    frames = ("clip", "zl", "x")
    tm = ("zl", "x")
    mp = ("zh", "core")
    in_specs = (
        P(frames, None),
        P(frames, None),
        P(tm, None, None),
        P(),
        P(mp, None),
        P(),
        P(),
        P(None, None, mp),
        P(mp, None),
    )
    out_specs = (P(frames, None, mp), P(frames, None), P("clip"))
    return jax.shard_map(body, mesh=finer, in_specs=in_specs, out_specs=out_specs, check_vma=False)
```
